32 devices in a mesh: horiz: 4 (over y, x), depth: 8 (over z, core).
Axes of the slice: x: 2, y: 2, z: 4, core: 2. Of those that a mesh axis runs over, the one named last changes fastest.
Arguments:
- fields: float32 [3, 256, 128, 256], P(None, 'depth', 'horiz'), may hold values from -6 to 6
- diffusivity: float32 [256, 128, 256], P('depth', 'horiz'), may hold values from 0.05 to 0.24
- offsets: int32 [128], P('horiz'), may hold values from 0 to 3
- coupling: float32 [4, 256], P(None, 'depth'), may hold values from 200 to 1600, as said below
- inverse: float32 [4, 256, 32], P(None, 'depth'), as said below
Outputs:
- advanced: float32 [3, 256, 128, 256], P(None, 'depth', 'horiz')
The draws below stay inside these ranges and needn't reach their ends.
Inputs may be any that keep to these rules, and one draw needn't show every extreme that they name: coupling[o, k] = coupling[0, k + o] wherever both exist. inverse[o, r * 32 + i, j] is entry (i, j) of the inverse of a block matrix: on the levels k of block r it has diagonal 1 + coupling[o, k] + coupling[o, k + 1] (the first term 0 for k = 0, the second 0 for k = 255) and -coupling[o, k] between levels k - 1 and k; in every block, row and column 31 are those of the identity.
All inputs are finite; a program needn't handle non-finite values.
Results may differ from the reference program's by a relative error of at most 0.0003.
Values sent between devices are 32-bit elements; how exact they have to be, the bound alone decides.
No kernel may reach another device: no remote copies, remote signals or barrier semaphores. Data moves between devices by JAX's collectives and lax.ppermute only.
A program may use at most 64 MiB of HBM per device.

```python
import jax
import jax.numpy as jnp
from jax import lax

LEV_DEV = 32
NY = 256
NOFF = 4
NZ = 256
NX = 128


def coupling_profile(key):
    base_key = jax.random.fold_in(key, 4211)
    profile = jnp.exp(jax.random.uniform(base_key, (NZ + NOFF,), jnp.float32, jnp.log(200.0), jnp.log(1600.0)))
    places = jnp.arange(NOFF)[:, None] + jnp.arange(NZ)[None, :]
    return profile[places]


def draw_coupling(key, part):
    return coupling_profile(key)


def draw_inverse(key, part):
    table = coupling_profile(key)
    level_count = LEV_DEV
    blocks = NZ // level_count
    levels_now = jnp.arange(NZ).reshape(blocks, level_count)
    lower_part = jnp.where(levels_now[None] > 0, table.reshape(NOFF, blocks, level_count), 0.0)
    upper_table = jnp.concatenate([table[:, 1:], jnp.zeros((NOFF, 1), jnp.float32)], axis=1)
    upper_part = upper_table.reshape(NOFF, blocks, level_count)
    main_part = 1.0 + lower_part + upper_part
    unit = jnp.eye(level_count, dtype=jnp.float32)
    below_unit = jnp.eye(level_count, k=-1, dtype=jnp.float32)
    above_unit = jnp.eye(level_count, k=1, dtype=jnp.float32)
    matrix = main_part[..., :, None] * unit - lower_part[..., :, None] * below_unit - upper_part[..., :, None] * above_unit
    last_mark = (jnp.arange(level_count) == level_count - 1).astype(jnp.float32)
    keep_mark = 1.0 - last_mark
    cut_matrix = matrix * keep_mark[:, None] * keep_mark[None, :] + last_mark[:, None] * last_mark[None, :]
    inverted = jnp.linalg.inv(cut_matrix)
    return inverted.reshape(NOFF, NZ, level_count).astype(jnp.float32)


def place_ends(drawn, own_key, smallest, largest):
    index_at = [jax.random.randint(jax.random.fold_in(own_key, axis), (), 0, length) for axis, length in enumerate(drawn.shape)]
    longest = drawn.shape.index(max(drawn.shape))
    neighbour = index_at[:longest] + [(index_at[longest] + 1) % drawn.shape[longest]] + index_at[longest + 1:]
    return drawn.at[tuple(index_at)].set(smallest).at[tuple(neighbour)].set(largest)


def block_levels(own_key, shape, cuts, low, top_value):
    level, own = 1.0, jax.random.fold_in(own_key, 6)
    for axis_at, parts in cuts:
        heights = jnp.exp(jax.random.uniform(jax.random.fold_in(own, axis_at), (parts,), jnp.float32, low / len(cuts), top_value / len(cuts)))
        level = level * jnp.repeat(heights, shape[axis_at] // parts).reshape([-1 if axis == axis_at else 1 for axis in range(len(shape))])
    return level


def scatter_about(key, shape, width, bound, split=(), kind=jnp.bfloat16):
    result = width * jax.random.normal(key, shape, jnp.float32)
    if split:
        result = result * block_levels(key, shape, split, -0.22, 0.18)
    return jnp.clip(result, -bound, bound).astype(kind)


def setup_inputs(seed: int = 0) -> dict:
    splits = jax.random.split(jax.random.key(seed), 6)
    return {
        "fields": scatter_about(splits[0], (3, NZ, NX, NY), 1.0, 6.0, ((1, 8), (2, 4)), jnp.float32),
        "diffusivity": jnp.clip(0.05 + 0.19 * jax.random.uniform(splits[1], (NZ, NX, NY), jnp.float32) ** block_levels(splits[1], (NZ, NX, NY), ((0, 8), (1, 4)), -0.2, 0.2), 0.05, 0.24),
        "offsets": place_ends(jax.random.randint(splits[2], (NX,), 0, NOFF), jax.random.fold_in(splits[2], 1), 0, NOFF - 1).astype(jnp.int32),
        "coupling": draw_coupling(jax.random.fold_in(splits[5], 71), 0),
        "inverse": draw_inverse(jax.random.fold_in(splits[5], 71), 0),
    }


exact_mode = lax.Precision.HIGHEST
wave_gain = 0.5

def tendency(centre, east_side, west_side, diffusivity):
    north_side = jnp.roll(centre, -1, axis=3)
    south_side = jnp.roll(centre, 1, axis=3)
    laplace = east_side + west_side + north_side + south_side - 4.0 * centre
    slope_along = 0.5 * (east_side - west_side)
    slope_across = 0.5 * (north_side - south_side)
    pushed = centre + diffusivity[None] * laplace
    first_part = pushed[0] - wave_gain * slope_along[2]
    second_part = pushed[1] - wave_gain * slope_across[2]
    third_part = pushed[2] - wave_gain * (slope_along[0] + slope_across[1])
    return jnp.stack([first_part, second_part, third_part])

def eliminate(level_slab, inverse_rows, coupling_rows, selector, block_index, blocks):
    chosen = jnp.einsum('jo,oab->jab', selector, inverse_rows, precision=exact_mode)
    line_coupling = jnp.dot(selector, coupling_rows, precision=exact_mode)
    solved = jnp.einsum('jab,fbjy->fajy', chosen, level_slab, precision=exact_mode)
    below_face = line_coupling[:, 0]
    upper_gate = line_coupling[:, -1]
    lower_gate = jnp.where(block_index > 0, below_face, jnp.zeros_like(below_face))
    spike_low = chosen[:, :, 0] * lower_gate[:, None]
    spike_high = chosen[:, :, -2] * upper_gate[:, None]
    return (solved, spike_low, spike_high, below_face, upper_gate)

def interface_rows(solved, spike_low, spike_high, upper_gate, got_rows, got_lines):
    lower_band = -upper_gate * spike_low[:, -2]
    main_band = 1.0 + upper_gate + got_lines[0] - upper_gate * spike_high[:, -2] - got_lines[1]
    upper_band = -got_lines[2]
    target = solved[:, -1] + upper_gate[None, :, None] * solved[:, -2] + got_rows
    return (lower_band, main_band, upper_band, target)

def thomas(lower_band, main_band, upper_band, target):

    def forward_step(state_now, row_data):
        prev_ratio, prev_value = state_now
        low_row, main_row, up_row, target_row = row_data
        pivot_value = main_row - low_row * prev_ratio
        ratio_now = up_row / pivot_value
        value_now = (target_row - low_row[None, :, None] * prev_value) / pivot_value[None, :, None]
        return ((ratio_now, value_now), (ratio_now, value_now))
    anchor = jnp.zeros_like(target[0])
    start_ratio = jnp.zeros_like(main_band[0])
    _, (ratios, values) = lax.scan(forward_step, (start_ratio, anchor), (lower_band, main_band, upper_band, target))

    def backward_step(next_value, row_data):
        ratio_now, value_now = row_data
        result_now = value_now - ratio_now[None, :, None] * next_value
        return (result_now, result_now)
    _, results = lax.scan(backward_step, anchor, (ratios, values), reverse=True)
    return results

def assemble(solved, spike_low, spike_high, previous, self_value):
    lifted = solved + spike_low.T[None, :, :, None] * previous[:, None] + spike_high.T[None, :, :, None] * self_value[:, None]
    return jnp.concatenate([lifted[:, :-1], self_value[:, None]], axis=1)

def solve_columns(slab_at, inverse, coupling, selector, total_levels):
    level_count = inverse.shape[2]
    blocks = total_levels // level_count

    def one_block(block_index):
        start_level = block_index * level_count
        level_slab = slab_at(start_level, level_count)
        inverse_rows = lax.dynamic_slice_in_dim(inverse, start_level, level_count, 1)
        coupling_rows = lax.dynamic_slice_in_dim(coupling, start_level, level_count, 1)
        return eliminate(level_slab, inverse_rows, coupling_rows, selector, block_index, blocks)
    solved, spike_low, spike_high, below_face, upper_gate = lax.map(one_block, jnp.arange(blocks, dtype=jnp.int32))
    send_lines = jnp.stack([below_face, below_face * spike_low[:, :, 0], below_face * spike_high[:, :, 0]], axis=1)
    send_rows = below_face[:, None, :, None] * solved[:, :, 0]
    got_lines = jnp.concatenate([send_lines[1:], jnp.zeros_like(send_lines[:1])], axis=0)
    got_rows = jnp.concatenate([send_rows[1:], jnp.zeros_like(send_rows[:1])], axis=0)
    lower_band, main_band, upper_band, target = jax.vmap(interface_rows)(solved, spike_low, spike_high, upper_gate, got_rows, got_lines)
    interfaces = thomas(lower_band, main_band, upper_band, target)
    previous = jnp.concatenate([jnp.zeros_like(interfaces[:1]), interfaces[:-1]], axis=0)
    columns = jax.vmap(assemble)(solved, spike_low, spike_high, previous, interfaces)
    shape_now = columns.shape
    return jnp.moveaxis(columns, 0, 1).reshape(shape_now[1], blocks * level_count, shape_now[3], shape_now[4])

def reference(fields, diffusivity, offsets, coupling, inverse):
    selector = (offsets[:, None] == jnp.arange(inverse.shape[0], dtype=jnp.int32)[None, :]).astype(jnp.float32)

    def slab_at(start_level, level_count):
        centre = lax.dynamic_slice_in_dim(fields, start_level, level_count, 1)
        heat_slab = lax.dynamic_slice_in_dim(diffusivity, start_level, level_count, 0)
        return tendency(centre, jnp.roll(centre, -1, axis=2), jnp.roll(centre, 1, axis=2), heat_slab)
    return solve_columns(slab_at, inverse, coupling, selector, fields.shape[1])
```

```python
import functools

import jax
import jax.numpy as jnp
from jax import lax
from jax.experimental import pallas as pl
from jax.experimental.pallas import tpu as pltpu
from jax.sharding import PartitionSpec as P

wave_gain = 0.5
SUB = 8
LANE = 128
VMEM = pltpu.VMEM
F32 = jnp.float32
BF16 = jnp.bfloat16


def vmem_spec():
    return pl.BlockSpec(memory_space=VMEM)


def choose(offs, rows):
    value = jnp.broadcast_to(rows[0], offs.shape)
    for o in range(1, len(rows)):
        value = jnp.where(offs == o, jnp.broadcast_to(rows[o], offs.shape), value)
    return value


def split_bf16(x):
    high = x.astype(BF16)
    low = (x - high.astype(F32)).astype(BF16)
    return high, low


def table_kernel(offs_ref, coupling_ref, inverse_ref, big_ref, offsb_ref, spikes_ref, coefs_ref, wide_ref):
    count, levels, _ = inverse_ref.shape
    lines = offsb_ref.shape[0]
    groups = lines // SUB
    rank = lax.axis_index("depth")

    for g in range(groups):
        sub = lax.broadcasted_iota(jnp.int32, (SUB, LANE), 0)
        value = jnp.zeros((SUB, LANE), jnp.int32)
        for j in range(SUB):
            value = jnp.where(sub == j, offs_ref[g * SUB + j], value)
        offsb_ref[g * SUB : (g + 1) * SUB, :] = value

    for o in range(count):
        gate = jnp.broadcast_to(coupling_ref[o : o + 1, levels - 1 : levels], (1, LANE))
        face = jnp.broadcast_to(coupling_ref[o : o + 1, 0:1], (1, LANE))
        face = jnp.where(rank > 0, face, jnp.zeros_like(face))
        low = jnp.broadcast_to(inverse_ref[o, :, 0:1], (levels, LANE)) * face
        high = jnp.broadcast_to(inverse_ref[o, :, levels - 2 : levels - 1], (levels, LANE)) * gate
        spikes_ref[0, o] = low
        spikes_ref[1, o] = high
        b = face - face * low[0:1]
        e = -face * high[0:1]
        l = -gate * low[levels - 2 : levels - 1]
        a = 1.0 + gate - gate * high[levels - 2 : levels - 1]
        for c, row in enumerate((b, e, l, a, gate, face)):
            coefs_ref[c * count + o : c * count + o + 1, :] = row

    width = levels * SUB
    spread = (
        lax.broadcasted_iota(jnp.int32, (levels, width), 1) // SUB
        == lax.broadcasted_iota(jnp.int32, (levels, width), 0)
    ).astype(F32)
    for o in range(count):
        wide_ref[o] = lax.dot_general(
            inverse_ref[o],
            spread,
            (((1,), (0,)), ((), ())),
            precision=lax.Precision.HIGHEST,
            preferred_element_type=F32,
        )
    lane = lax.broadcasted_iota(jnp.int32, (SUB, width), 1)
    sub = lax.broadcasted_iota(jnp.int32, (SUB, width), 0)
    diagonal = lane % SUB == sub
    zero = jnp.zeros((SUB, width), F32)
    offs_wide = [
        jnp.concatenate([offsb_ref[g * SUB : (g + 1) * SUB, :]] * (width // LANE), axis=1) for g in range(groups)
    ]

    def one_pair(k, _):
        rows = [[wide_ref[o, pl.ds(2 * k + i, 1), :] for o in range(count)] for i in range(2)]
        for g in range(groups):
            both = jnp.concatenate(
                [jnp.where(diagonal, choose(offs_wide[g], rows[i]), zero) for i in range(2)], axis=0
            )
            high, low = split_bf16(both)
            at = pl.multiple_of(k * 2 * SUB, 2 * SUB)
            big_ref[g, 0, pl.ds(at, 2 * SUB), :] = high
            big_ref[g, 1, pl.ds(at, 2 * SUB), :] = low
        return 0

    lax.fori_loop(0, levels // 2, one_pair, 0)


def forcing_kernel(
    fields_ref, diff_ref, west_ref, east_ref, big_ref, offsb_ref, coefs_ref, solved_ref, send_ref, keep_ref, work_ref
):
    parts, levels, lines, ny = fields_ref.shape
    groups = lines // SUB
    half = ny // 2
    count = coefs_ref.shape[0] // 6
    core = lax.axis_index("depth") % 2
    sub = lax.broadcasted_iota(jnp.int32, (SUB, ny), 0)

    for g in range(groups):
        first = g * SUB

        def one_level(k, _):
            centre, across, along, both = [], [], [], []
            for i in range(parts):
                c = fields_ref[i, k, first : first + SUB, :]
                north = pltpu.roll(c, ny - 1, 1)
                south = pltpu.roll(c, 1, 1)
                if g > 0:
                    row_w = fields_ref[i, k, first - 1 : first, :]
                else:
                    row_w = west_ref[i, pl.ds(k, 1), :]
                if g < groups - 1:
                    row_e = fields_ref[i, k, first + SUB : first + SUB + 1, :]
                else:
                    row_e = east_ref[i, pl.ds(k, 1), :]
                east = jnp.where(sub == SUB - 1, jnp.broadcast_to(row_e, c.shape), pltpu.roll(c, SUB - 1, 0))
                west = jnp.where(sub == 0, jnp.broadcast_to(row_w, c.shape), pltpu.roll(c, 1, 0))
                centre.append(c)
                both.append((east + west) + (north + south) - 4.0 * c)
                along.append(east - west)
                across.append(north - south)
            d = diff_ref[k, first : first + SUB, :]
            scale = 0.5 * wave_gain
            out = (
                centre[0] + d * both[0] - scale * along[2],
                centre[1] + d * both[1] - scale * across[2],
                centre[2] + d * both[2] - scale * (along[0] + across[1]),
            )
            at = pl.multiple_of(k * SUB, SUB)
            for i in range(parts):
                work_ref[i, pl.ds(at, SUB), :] = out[i]
            return 0

        lax.fori_loop(0, levels, one_level, 0, unroll=4)
        offs = offsb_ref[first : first + SUB, :]
        gate = choose(offs, [coefs_ref[4 * count + o : 4 * count + o + 1, :] for o in range(count)])
        face = choose(offs, [coefs_ref[5 * count + o : 5 * count + o + 1, :] for o in range(count)])
        for i in range(parts):
            x_high, x_low = split_bf16(work_ref[i])
            m_high = big_ref[g, 0]
            m_low = big_ref[g, 1]
            result = (
                jnp.dot(m_high, x_high, preferred_element_type=F32)
                + jnp.dot(m_low, x_high, preferred_element_type=F32)
                + jnp.dot(m_high, x_low, preferred_element_type=F32)
            )
            solved_ref[i, :, first : first + SUB, :] = result.reshape(levels, SUB, ny)
            last = result[(levels - 1) * SUB :, :]
            before = result[(levels - 2) * SUB : (levels - 1) * SUB, :]
            top = result[:SUB, :]
            for h in range(2):
                cut = slice(h * half, (h + 1) * half)
                a_side = last[:, cut] + gate * before[:, cut]
                b_side = face * top[:, cut]
                for k, value in enumerate((a_side, b_side)):
                    at = (k * parts + i) * lines + first

                    @pl.when(core == h)
                    def _():
                        keep_ref[at : at + SUB, :] = value

                    @pl.when(core != h)
                    def _():
                        send_ref[at : at + SUB, :] = value

    base = 2 * parts * lines
    send_ref[base : base + 4 * count, :] = coefs_ref[: 4 * count, :]
    keep_ref[base : base + 4 * count, :] = coefs_ref[: 4 * count, :]


def unpack(ref, rows, count):
    a_side = ref[:rows, :]
    b_side = ref[rows : 2 * rows, :]
    base = 2 * rows
    b, e, l, a = [ref[base + c * count : base + (c + 1) * count, :] for c in range(4)]
    return a_side, b_side, b, e, l, a


def per_line(offs, table, parts):
    rows = [table[o : o + 1, :] for o in range(table.shape[0])]
    value = choose(offs, rows)
    return jnp.concatenate([value] * parts, axis=0)


def merged(bit, mine_ref, got_ref, offs, parts, count):
    lines = offs.shape[0]
    rows = parts * lines
    lower_is_mine = (lax.axis_index("depth") >> bit) % 2 == 0
    mine = unpack(mine_ref, rows, count)
    got = unpack(got_ref, rows, count)
    a_1, b_1, cb_1, ce_1, cl_1, ca_1 = [jnp.where(lower_is_mine, x, y) for x, y in zip(mine, got)]
    a_2, b_2, cb_2, ce_2, cl_2, ca_2 = [jnp.where(lower_is_mine, y, x) for x, y in zip(mine, got)]
    inverse = 1.0 / (ca_1 + cb_2)
    total = a_1 + b_2
    down = ce_1 * inverse
    up = cl_2 * inverse
    a_new = a_2 - per_line(offs, up, parts) * total
    b_new = b_1 - per_line(offs, down, parts) * total
    cb = cb_1 - down * cl_1
    ce = -down * ce_2
    cl = -up * cl_1
    ca = ca_2 - up * ce_2
    middle = per_line(offs, inverse, parts) * total
    return (a_new, b_new, cb, ce, cl, ca), (middle, cl_1 * inverse, ce_2 * inverse)


def store_saved(saved_ref, saved, count):
    middle, low, high = saved
    rows = middle.shape[0]
    saved_ref[:rows, :] = middle
    saved_ref[rows : rows + count, :] = low
    saved_ref[rows + count : rows + 2 * count, :] = high


def store_element(ref, element, count):
    rows = element[0].shape[0]
    ref[:rows, :] = element[0]
    ref[rows : 2 * rows, :] = element[1]
    for c in range(4):
        ref[2 * rows + c * count : 2 * rows + (c + 1) * count, :] = element[2 + c]


def merge_kernel(bit, parts, count, mine_ref, got_ref, offsb_ref, element_ref, saved_ref):
    element, saved = merged(bit, mine_ref, got_ref, offsb_ref[...], parts, count)
    store_element(element_ref, element, count)
    store_saved(saved_ref, saved, count)


def merge_last_kernel(bit, parts, count, mine_ref, got_ref, offsb_ref, element_ref, saved_ref, send_ref):
    offs = offsb_ref[...]
    element, saved = merged(bit, mine_ref, got_ref, offs, parts, count)
    store_element(element_ref, element, count)
    store_saved(saved_ref, saved, count)
    a_side, b_side, cb, ce, cl, ca = element
    rows = a_side.shape[0]
    lower = (lax.axis_index("depth") >> (bit + 1)) == 0
    ratio = ce / ca
    send_ref[:rows, :] = jnp.where(lower, a_side, b_side - per_line(offs, ratio, parts) * a_side)
    send_ref[rows : rows + count, :] = jnp.where(lower, ca, cb - ratio * cl)


def solve_kernel(bits, parts, count, *refs):
    sent_ref, got_ref, element_ref, offsb_ref = refs[:4]
    saved_refs = refs[4 : 4 + bits]
    send_ref, keep_ref = refs[4 + bits :]
    offs = offsb_ref[...]
    rows = parts * offs.shape[0]
    rank = lax.axis_index("depth")
    pivot = sent_ref[rows : rows + count, :] + got_ref[rows : rows + count, :]
    shared = (sent_ref[:rows, :] + got_ref[:rows, :]) * per_line(offs, 1.0 / pivot, parts)
    a_side, _, _, _, cl, ca = unpack(element_ref, rows, count)
    inverse = 1.0 / ca
    top = per_line(offs, inverse, parts) * a_side - per_line(offs, cl * inverse, parts) * shared
    lower = (rank >> bits) == 0
    below = jnp.where(lower, jnp.zeros_like(shared), shared)
    above = jnp.where(lower, shared, top)
    for bit in reversed(range(bits)):
        saved_ref = saved_refs[bit]
        low = saved_ref[rows : rows + count, :]
        high = saved_ref[rows + count : rows + 2 * count, :]
        middle = saved_ref[:rows, :] - per_line(offs, low, parts) * below - per_line(offs, high, parts) * above
        lower = (rank >> bit) % 2 == 0
        if bit > 0:
            below, above = jnp.where(lower, below, middle), jnp.where(lower, middle, above)
        else:
            keep_ref[:rows, :] = jnp.where(lower, below, middle)
            keep_ref[rows:, :] = jnp.where(lower, middle, above)
            send_ref[:rows, :] = jnp.where(lower, middle, below)
            send_ref[rows:, :] = jnp.where(lower, above, middle)


def finish_kernel(solved_ref, own_ref, other_ref, offsb_ref, spikes_ref, out_ref):
    parts, levels, lines, ny = solved_ref.shape
    groups = lines // SUB
    half = ny // 2
    count = spikes_ref.shape[1]
    rows = parts * lines
    core = lax.axis_index("depth") % 2
    for g in range(groups):
        first = g * SUB
        offs = offsb_ref[first : first + SUB, :]
        ends = []
        for k in range(2):
            for i in range(parts):
                at = k * rows + i * lines + first
                own = own_ref[at : at + SUB, :]
                other = other_ref[at : at + SUB, :]
                ends.append((jnp.where(core == 0, own, other), jnp.where(core == 0, other, own)))

        def one_level(k, _):
            low = choose(offs, [spikes_ref[0, o, pl.ds(k, 1), :] for o in range(count)])
            high = choose(offs, [spikes_ref[1, o, pl.ds(k, 1), :] for o in range(count)])
            for i in range(parts):
                for h in range(2):
                    cut = slice(h * half, (h + 1) * half)
                    value = solved_ref[i, k, first : first + SUB, cut]
                    out_ref[i, k, first : first + SUB, cut] = (
                        value + low * ends[i][h] + high * ends[parts + i][h]
                    )
            return 0

        lax.fori_loop(0, levels - 1, one_level, 0, unroll=2)
        for i in range(parts):
            for h in range(2):
                cut = slice(h * half, (h + 1) * half)
                out_ref[i, levels - 1, first : first + SUB, cut] = ends[parts + i][h]


def call(kernel, outs, args, scratch=(), specs=None):
    return pl.pallas_call(
        kernel,
        out_shape=[jax.ShapeDtypeStruct(s, d) for s, d in outs],
        in_specs=specs or [vmem_spec()] * len(args),
        out_specs=[vmem_spec()] * len(outs),
        scratch_shapes=list(scratch),
    )(*args)


def body(fields, diffusivity, offsets, coupling, inverse):
    parts, levels, lines, ny = fields.shape
    count = inverse.shape[0]
    half = ny // 2
    groups = lines // SUB
    width = levels * SUB
    around = lax.axis_size("horiz")
    ranks = lax.axis_size("depth")
    bits = ranks.bit_length() - 1
    assert ranks == 1 << bits and bits >= 2 and half == LANE

    def swap(x, bit):
        return lax.ppermute(x, "depth", [(i, i ^ (1 << bit)) for i in range(ranks)])

    forward = [(i, (i + 1) % around) for i in range(around)]
    backward = [(i, (i - 1) % around) for i in range(around)]
    west = lax.ppermute(fields[:, :, lines - 1, :], "horiz", forward)
    east = lax.ppermute(fields[:, :, 0, :], "horiz", backward)

    big, offsb, spikes, coefs = call(
        table_kernel,
        [
            ((groups, 2, width, width), BF16),
            ((lines, LANE), jnp.int32),
            ((2, count, levels, LANE), F32),
            ((6 * count, LANE), F32),
        ],
        (offsets, coupling, inverse),
        scratch=[pltpu.VMEM((count, levels, width), F32)],
        specs=[pl.BlockSpec(memory_space=pltpu.SMEM), vmem_spec(), vmem_spec()],
    )
    rows = parts * lines
    element_shape = ((2 * rows + 4 * count, half), F32)
    saved_shape = ((rows + 2 * count, half), F32)
    solved, send, keep = call(
        forcing_kernel,
        [((parts, levels, lines, ny), F32), element_shape, element_shape],
        (fields, diffusivity, west, east, big, offsb, coefs),
        scratch=[pltpu.VMEM((parts, width, ny), F32)],
    )
    got = swap(send, 0)
    mine = keep
    saved = []
    for bit in range(bits - 1):
        if bit < bits - 2:
            mine, kept = call(
                functools.partial(merge_kernel, bit, parts, count),
                [element_shape, saved_shape],
                (mine, got, offsb),
            )
            got = swap(mine, bit + 1)
        else:
            mine, kept, send = call(
                functools.partial(merge_last_kernel, bit, parts, count),
                [element_shape, saved_shape, ((rows + count, half), F32)],
                (mine, got, offsb),
            )
            got = swap(send, bit + 1)
        saved.append(kept)
    pair = ((2 * rows, half), F32)
    theirs, own = call(
        functools.partial(solve_kernel, bits - 1, parts, count),
        [pair, pair],
        (send, got, mine, offsb, *saved),
    )
    other = swap(theirs, 0)
    (out,) = call(
        finish_kernel,
        [((parts, levels, lines, ny), F32)],
        (solved, own, other, offsb, spikes),
    )
    return out


def solution(mesh):
    return jax.shard_map(
        body,
        mesh=mesh,
        in_specs=(
            P(None, "depth", "horiz", None),
            P("depth", "horiz", None),
            P("horiz"),
            P(None, "depth"),
            P(None, "depth", None),
        ),
        out_specs=P(None, "depth", "horiz", None),
        check_vma=False,
    )
```

```python
import functools

import jax
import jax.numpy as jnp
from jax import lax
from jax.experimental import pallas as pl
from jax.experimental.pallas import tpu as pltpu
from jax.sharding import PartitionSpec as P

wave_gain = 0.5
SUB = 8
LANE = 128
VMEM = pltpu.VMEM
F32 = jnp.float32
BF16 = jnp.bfloat16


def vmem_spec():
    return pl.BlockSpec(memory_space=VMEM)


def choose(offs, rows):
    value = jnp.broadcast_to(rows[0], offs.shape)
    for o in range(1, len(rows)):
        value = jnp.where(offs == o, jnp.broadcast_to(rows[o], offs.shape), value)
    return value


def split_bf16(x):
    high = x.astype(BF16)
    low = (x - high.astype(F32)).astype(BF16)
    return high, low


def outermost_kernel(fields_ref, first_ref, last_ref, stage_ref, sems):
    parts, levels, lines, ny = fields_ref.shape
    copies = []
    for e, start in enumerate((0, lines - SUB)):
        copy = pltpu.make_async_copy(fields_ref.at[:, :, pl.ds(start, SUB), :], stage_ref.at[e], sems.at[e])
        copy.start()
        copies.append(copy)
    sub = lax.broadcasted_iota(jnp.int32, (SUB, ny), 0)
    for e, (line, ref) in enumerate(((0, first_ref), (SUB - 1, last_ref))):
        copies[e].wait()
        for i in range(parts):
            for c in range(levels // SUB):
                value = jnp.zeros((SUB, ny), F32)
                for t in range(SUB):
                    row = stage_ref[e, i, c * SUB + t, line : line + 1, :]
                    value = jnp.where(sub == t, jnp.broadcast_to(row, value.shape), value)
                ref[i, c * SUB : (c + 1) * SUB, :] = value


def fill_tables(offs_ref, coupling_ref, inverse_ref, offsb_ref, spikes_ref, rows_ref, coefs_ref):
    count, levels, _ = inverse_ref.shape
    lines = offsb_ref.shape[0]
    rank = lax.axis_index("depth")

    sub = lax.broadcasted_iota(jnp.int32, (SUB, LANE), 0)
    for g in range(lines // SUB):
        value = jnp.zeros((SUB, LANE), jnp.int32)
        for j in range(SUB):
            value = jnp.where(sub == j, offs_ref[g * SUB + j], value)
        offsb_ref[g * SUB : (g + 1) * SUB, :] = value

    eye = lax.broadcasted_iota(jnp.int32, (levels, levels), 0) == lax.broadcasted_iota(
        jnp.int32, (levels, levels), 1
    )
    for o in range(count):
        gate = jnp.broadcast_to(coupling_ref[o : o + 1, levels - 1 : levels], (1, LANE))
        face = jnp.broadcast_to(coupling_ref[o : o + 1, 0:1], (1, LANE))
        face = jnp.where(rank > 0, face, jnp.zeros_like(face))
        low = jnp.broadcast_to(inverse_ref[o, :, 0:1], (levels, LANE)) * face
        high = jnp.broadcast_to(inverse_ref[o, :, levels - 2 : levels - 1], (levels, LANE)) * gate
        spikes_ref[0, o] = low
        spikes_ref[1, o] = high
        for k, level in enumerate((0, levels - 2)):
            row = jnp.broadcast_to(inverse_ref[o, level : level + 1, :], (levels, levels))
            column = jnp.sum(jnp.where(eye, row, jnp.zeros_like(row)), axis=1, keepdims=True)
            rows_ref[k, o] = jnp.broadcast_to(column, (levels, LANE))
        b = face - face * low[0:1]
        e = -face * high[0:1]
        l = -gate * low[levels - 2 : levels - 1]
        a = 1.0 + gate - gate * high[levels - 2 : levels - 1]
        for c, row in enumerate((b, e, l, a, gate, face)):
            coefs_ref[c * count + o : c * count + o + 1, :] = row


def force_group(
    g, slot, stages, fields_ref, diff_ref, west_ref, east_ref, offsb_ref, rows_ref, coefs_ref, forcing_ref, sides_ref
):
    parts, levels, lines, ny = fields_ref.shape
    groups = lines // SUB
    half = ny // 2
    count = rows_ref.shape[1]
    first = g * SUB
    sub = lax.broadcasted_iota(jnp.int32, (SUB, ny), 0)
    offs = offsb_ref[first : first + SUB, :]
    gate = choose(offs, [coefs_ref[4 * count + o : 4 * count + o + 1, :] for o in range(count)])
    face = choose(offs, [coefs_ref[5 * count + o : 5 * count + o + 1, :] for o in range(count)])

    def one_level(k, sums):
        centre, across, along, both = [], [], [], []
        for i in range(parts):
            c = fields_ref[i, k, first : first + SUB, :]
            north = pltpu.roll(c, ny - 1, 1)
            south = pltpu.roll(c, 1, 1)
            if g > 0:
                row_w = fields_ref[i, k, first - 1 : first, :]
            else:
                row_w = west_ref[i, pl.ds(k, 1), :]
            if g < groups - 1:
                row_e = fields_ref[i, k, first + SUB : first + SUB + 1, :]
            else:
                row_e = east_ref[i, pl.ds(k, 1), :]
            east = jnp.where(sub == SUB - 1, jnp.broadcast_to(row_e, c.shape), pltpu.roll(c, SUB - 1, 0))
            west = jnp.where(sub == 0, jnp.broadcast_to(row_w, c.shape), pltpu.roll(c, 1, 0))
            centre.append(c)
            both.append((east + west) + (north + south) - 4.0 * c)
            along.append(east - west)
            across.append(north - south)
        d = diff_ref[k, first : first + SUB, :]
        scale = 0.5 * wave_gain
        out = (
            centre[0] + d * both[0] - scale * along[2],
            centre[1] + d * both[1] - scale * across[2],
            centre[2] + d * both[2] - scale * (along[0] + across[1]),
        )
        at = pl.multiple_of(k * SUB, SUB)
        top = choose(offs, [rows_ref[0, o, pl.ds(k, 1), :] for o in range(count)])
        bottom = choose(offs, [rows_ref[1, o, pl.ds(k, 1), :] for o in range(count)])
        new = []
        for i in range(parts):
            forcing_ref[slot, i, pl.ds(at, SUB), :] = out[i]
            for h in range(2):
                piece = out[i][:, h * half : (h + 1) * half]
                at_0, at_1 = sums[2 * (i * 2 + h)], sums[2 * (i * 2 + h) + 1]
                new += [at_0 + top * piece, at_1 + bottom * piece]
        return tuple(new)

    sums = tuple(jnp.zeros((SUB, half), F32) for _ in range(4 * parts))
    step = levels // len(stages)
    for c, wait in enumerate(stages):
        wait()
        sums = lax.fori_loop(c * step, (c + 1) * step, one_level, sums, unroll=step)
    for i in range(parts):
        for h in range(2):
            cut = slice(h * half, (h + 1) * half)
            last = forcing_ref[slot, i, (levels - 1) * SUB :, cut]
            sides_ref[0, i, slot, :, cut] = last + gate * sums[2 * (i * 2 + h) + 1]
            sides_ref[1, i, slot, :, cut] = face * sums[2 * (i * 2 + h)]


def nothing():
    pass


def inner_kernel(
    fields_hbm,
    diff_hbm,
    offs_ref,
    coupling_ref,
    inverse_ref,
    fields_ref,
    diff_ref,
    offsb_ref,
    spikes_ref,
    rows_ref,
    coefs_ref,
    forcing_ref,
    sides_ref,
    sems,
):
    parts, levels, lines, _ = fields_ref.shape
    groups = lines // SUB
    chunks = sems.shape[0] // (parts + 1)
    step = levels // chunks
    waits = []
    for c in range(chunks):
        at = pl.ds(c * step, step)
        copies = [
            pltpu.make_async_copy(fields_hbm.at[i, at], fields_ref.at[i, at], sems.at[c * (parts + 1) + i])
            for i in range(parts)
        ]
        copies.append(pltpu.make_async_copy(diff_hbm.at[at], diff_ref.at[at], sems.at[c * (parts + 1) + parts]))
        for copy in copies:
            copy.start()
        waits.append(lambda copies=copies: [copy.wait() for copy in copies])
    fill_tables(offs_ref, coupling_ref, inverse_ref, offsb_ref, spikes_ref, rows_ref, coefs_ref)
    for slot, g in enumerate(range(1, groups - 1)):
        force_group(
            g,
            slot,
            waits if slot == 0 else [nothing] * chunks,
            fields_ref,
            diff_ref,
            None,
            None,
            offsb_ref,
            rows_ref,
            coefs_ref,
            forcing_ref,
            sides_ref,
        )


def edge_kernel(
    fields_ref,
    diff_ref,
    west_ref,
    east_ref,
    offsb_ref,
    rows_ref,
    coefs_ref,
    inner_ref,
    forcing_ref,
    send_ref,
    keep_ref,
    sides_ref,
):
    parts, levels, lines, ny = fields_ref.shape
    groups = lines // SUB
    half = ny // 2
    count = rows_ref.shape[1]
    core = lax.axis_index("depth") % 2
    for slot, g in enumerate((0, groups - 1)):
        force_group(
            g,
            slot,
            [nothing] * (levels // SUB),
            fields_ref,
            diff_ref,
            west_ref,
            east_ref,
            offsb_ref,
            rows_ref,
            coefs_ref,
            forcing_ref,
            sides_ref,
        )
    for g in range(groups):
        ref, slot = place(g, groups, inner_ref, sides_ref)
        for i in range(parts):
            for k in range(2):
                at = (k * parts + i) * lines + g * SUB
                left, right = ref[k, i, slot, :, :half], ref[k, i, slot, :, half:]
                keep_ref[at : at + SUB, :] = jnp.where(core == 0, left, right)
                send_ref[at : at + SUB, :] = jnp.where(core == 0, right, left)

    base = 2 * parts * lines
    send_ref[base : base + 4 * count, :] = coefs_ref[: 4 * count, :]
    keep_ref[base : base + 4 * count, :] = coefs_ref[: 4 * count, :]


def place(g, groups, inner_ref, outer_ref):
    if g == 0:
        return outer_ref, 0
    if g == groups - 1:
        return outer_ref, 1
    return inner_ref, g - 1


def block_kernel(after_ref, inner_ref, outer_ref, offsb_ref, inverse_ref, solved_ref, token_ref, wide_ref, big_ref):
    count, levels, _ = inverse_ref.shape
    groups, parts, width, ny = solved_ref.shape
    token_ref[...] = after_ref[:SUB, :]

    spread = (
        lax.broadcasted_iota(jnp.int32, (levels, width), 1) // SUB
        == lax.broadcasted_iota(jnp.int32, (levels, width), 0)
    ).astype(F32)
    for o in range(count):
        wide_ref[o] = lax.dot_general(
            inverse_ref[o],
            spread,
            (((1,), (0,)), ((), ())),
            precision=lax.Precision.HIGHEST,
            preferred_element_type=F32,
        )
    lane = lax.broadcasted_iota(jnp.int32, (SUB, width), 1)
    sub = lax.broadcasted_iota(jnp.int32, (SUB, width), 0)
    diagonal = lane % SUB == sub
    zero = jnp.zeros((SUB, width), F32)
    offs_wide = [
        jnp.concatenate([offsb_ref[g * SUB : (g + 1) * SUB, :]] * (width // LANE), axis=1) for g in range(groups)
    ]

    def one_pair(k, _):
        rows = [[wide_ref[o, pl.ds(2 * k + i, 1), :] for o in range(count)] for i in range(2)]
        for g in range(groups):
            both = jnp.concatenate(
                [jnp.where(diagonal, choose(offs_wide[g], rows[i]), zero) for i in range(2)], axis=0
            )
            high, low = split_bf16(both)
            at = pl.multiple_of(k * 2 * SUB, 2 * SUB)
            big_ref[g, 0, pl.ds(at, 2 * SUB), :] = high
            big_ref[g, 1, pl.ds(at, 2 * SUB), :] = low
        return 0

    lax.fori_loop(0, levels // 2, one_pair, 0)
    for g in range(groups):
        ref, slot = place(g, groups, inner_ref, outer_ref)
        m_high = big_ref[g, 0]
        m_low = big_ref[g, 1]
        for i in range(parts):
            x_high, x_low = split_bf16(ref[slot, i])
            solved_ref[g, i] = (
                jnp.dot(m_high, x_high, preferred_element_type=F32)
                + jnp.dot(m_low, x_high, preferred_element_type=F32)
                + jnp.dot(m_high, x_low, preferred_element_type=F32)
            )


def unpack(ref, rows, count):
    a_side = ref[:rows, :]
    b_side = ref[rows : 2 * rows, :]
    base = 2 * rows
    b, e, l, a = [ref[base + c * count : base + (c + 1) * count, :] for c in range(4)]
    return a_side, b_side, b, e, l, a


def per_line(offs, table, parts):
    rows = [table[o : o + 1, :] for o in range(table.shape[0])]
    value = choose(offs, rows)
    return jnp.concatenate([value] * parts, axis=0)


def merged(bit, mine_ref, got_ref, offs, parts, count):
    lines = offs.shape[0]
    rows = parts * lines
    lower_is_mine = (lax.axis_index("depth") >> bit) % 2 == 0
    mine = unpack(mine_ref, rows, count)
    got = unpack(got_ref, rows, count)
    a_1, b_1, cb_1, ce_1, cl_1, ca_1 = [jnp.where(lower_is_mine, x, y) for x, y in zip(mine, got)]
    a_2, b_2, cb_2, ce_2, cl_2, ca_2 = [jnp.where(lower_is_mine, y, x) for x, y in zip(mine, got)]
    inverse = 1.0 / (ca_1 + cb_2)
    total = a_1 + b_2
    down = ce_1 * inverse
    up = cl_2 * inverse
    a_new = a_2 - per_line(offs, up, parts) * total
    b_new = b_1 - per_line(offs, down, parts) * total
    cb = cb_1 - down * cl_1
    ce = -down * ce_2
    cl = -up * cl_1
    ca = ca_2 - up * ce_2
    middle = per_line(offs, inverse, parts) * total
    return (a_new, b_new, cb, ce, cl, ca), (middle, cl_1 * inverse, ce_2 * inverse)


def store_saved(saved_ref, saved, count):
    middle, low, high = saved
    rows = middle.shape[0]
    saved_ref[:rows, :] = middle
    saved_ref[rows : rows + count, :] = low
    saved_ref[rows + count : rows + 2 * count, :] = high


def store_element(ref, element, count):
    rows = element[0].shape[0]
    ref[:rows, :] = element[0]
    ref[rows : 2 * rows, :] = element[1]
    for c in range(4):
        ref[2 * rows + c * count : 2 * rows + (c + 1) * count, :] = element[2 + c]


def merge_kernel(bit, parts, count, mine_ref, got_ref, offsb_ref, element_ref, saved_ref):
    element, saved = merged(bit, mine_ref, got_ref, offsb_ref[...], parts, count)
    store_element(element_ref, element, count)
    store_saved(saved_ref, saved, count)


def merge_last_kernel(bit, parts, count, mine_ref, got_ref, offsb_ref, token_ref, element_ref, saved_ref, send_ref):
    offs = offsb_ref[...]
    element, saved = merged(bit, mine_ref, got_ref, offs, parts, count)
    store_element(element_ref, element, count)
    store_saved(saved_ref, saved, count)
    a_side, b_side, cb, ce, cl, ca = element
    rows = a_side.shape[0]
    lower = (lax.axis_index("depth") >> (bit + 1)) == 0
    ratio = ce / ca
    send_ref[:rows, :] = jnp.where(lower, a_side, b_side - per_line(offs, ratio, parts) * a_side)
    send_ref[rows : rows + count, :] = jnp.where(lower, ca, cb - ratio * cl)


def solve_kernel(bits, parts, count, *refs):
    sent_ref, got_ref, element_ref, offsb_ref = refs[:4]
    saved_refs = refs[4 : 4 + bits]
    send_ref, keep_ref = refs[4 + bits :]
    offs = offsb_ref[...]
    rows = parts * offs.shape[0]
    rank = lax.axis_index("depth")
    pivot = sent_ref[rows : rows + count, :] + got_ref[rows : rows + count, :]
    shared = (sent_ref[:rows, :] + got_ref[:rows, :]) * per_line(offs, 1.0 / pivot, parts)
    a_side, _, _, _, cl, ca = unpack(element_ref, rows, count)
    inverse = 1.0 / ca
    top = per_line(offs, inverse, parts) * a_side - per_line(offs, cl * inverse, parts) * shared
    lower = (rank >> bits) == 0
    below = jnp.where(lower, jnp.zeros_like(shared), shared)
    above = jnp.where(lower, shared, top)
    for bit in reversed(range(bits)):
        saved_ref = saved_refs[bit]
        low = saved_ref[rows : rows + count, :]
        high = saved_ref[rows + count : rows + 2 * count, :]
        middle = saved_ref[:rows, :] - per_line(offs, low, parts) * below - per_line(offs, high, parts) * above
        lower = (rank >> bit) % 2 == 0
        if bit > 0:
            below, above = jnp.where(lower, below, middle), jnp.where(lower, middle, above)
        else:
            keep_ref[:rows, :] = jnp.where(lower, below, middle)
            keep_ref[rows:, :] = jnp.where(lower, middle, above)
            send_ref[:rows, :] = jnp.where(lower, middle, below)
            send_ref[rows:, :] = jnp.where(lower, above, middle)


def finish_kernel(step, solved_ref, own_ref, other_ref, offsb_ref, spikes_ref, out_ref, stage_ref, sems):
    parts, levels, lines, ny = out_ref.shape
    groups = lines // SUB
    half = ny // 2
    count = spikes_ref.shape[1]
    rows = parts * lines
    core = lax.axis_index("depth") % 2

    def ends(g):
        values = []
        for k in range(2):
            for i in range(parts):
                at = k * rows + i * lines + g * SUB
                own = own_ref[at : at + SUB, :]
                other = other_ref[at : at + SUB, :]
                values.append((jnp.where(core == 0, own, other), jnp.where(core == 0, other, own)))
        return values

    copies = []
    for c in range(levels // step):
        for g in range(groups):
            lane = slice(g * SUB, (g + 1) * SUB)
            offs = offsb_ref[lane, :]
            side = ends(g)

            def one_level(k, _):
                at = pl.multiple_of(k * SUB, SUB)
                low = choose(offs, [spikes_ref[0, o, pl.ds(k, 1), :] for o in range(count)])
                high = choose(offs, [spikes_ref[1, o, pl.ds(k, 1), :] for o in range(count)])
                for i in range(parts):
                    for h in range(2):
                        cut = slice(h * half, (h + 1) * half)
                        stage_ref[i, k, lane, cut] = (
                            solved_ref[g, i, pl.ds(at, SUB), cut] + low * side[i][h] + high * side[parts + i][h]
                        )
                return 0

            stop = (c + 1) * step
            last = stop == levels
            lax.fori_loop(c * step, stop - 1 if last else stop, one_level, 0, unroll=True)
            if last:
                for i in range(parts):
                    for h in range(2):
                        cut = slice(h * half, (h + 1) * half)
                        stage_ref[i, levels - 1, lane, cut] = side[parts + i][h]
        for i in range(parts):
            at = pl.ds(c * step, step)
            copy = pltpu.make_async_copy(stage_ref.at[i, at], out_ref.at[i, at], sems.at[c * parts + i])
            copy.start()
            copies.append(copy)
    for copy in copies:
        copy.wait()


def call(kernel, outs, args, scratch=(), specs=None, keep=True):
    put = [pltpu.with_memory_space_constraint(x, VMEM) for x in args] if specs is None else args
    return pl.pallas_call(
        kernel,
        out_shape=[VMEM(s, d) if keep else jax.ShapeDtypeStruct(s, d) for s, d in outs],
        in_specs=specs or [vmem_spec()] * len(args),
        out_specs=[vmem_spec() if keep else pl.BlockSpec(memory_space=pl.ANY)] * len(outs),
        scratch_shapes=list(scratch),
        compiler_params=pltpu.CompilerParams(vmem_limit_bytes=16 * 2**20),
    )(*put)


def body(fields, diffusivity, offsets, coupling, inverse):
    parts, levels, lines, ny = fields.shape
    count = inverse.shape[0]
    half = ny // 2
    groups = lines // SUB
    width = levels * SUB
    around = lax.axis_size("horiz")
    ranks = lax.axis_size("depth")
    bits = ranks.bit_length() - 1
    assert ranks == 1 << bits and bits >= 2 and half == LANE and groups >= 3

    def swap(x, bit):
        return lax.ppermute(x, "depth", [(i, i ^ (1 << bit)) for i in range(ranks)])

    anywhere = pl.BlockSpec(memory_space=pltpu.HBM)
    fields = pltpu.with_memory_space_constraint(fields, pltpu.HBM)
    diffusivity = pltpu.with_memory_space_constraint(diffusivity, pltpu.HBM)
    edge = ((parts, levels, ny), F32)
    first, last = call(
        outermost_kernel,
        [edge, edge],
        (fields,),
        scratch=[pltpu.VMEM((2, parts, levels, SUB, ny), F32), pltpu.SemaphoreType.DMA((2,))],
        specs=[anywhere],
    )
    west = lax.ppermute(last, "horiz", [(i, (i + 1) % around) for i in range(around)])
    east = lax.ppermute(first, "horiz", [(i, (i - 1) % around) for i in range(around)])

    rows = parts * lines
    chunks = levels // SUB
    table = ((2, count, levels, LANE), F32)
    fields_v, diff_v, offsb, spikes, k_rows, coefs, inner, sides = call(
        inner_kernel,
        [
            (fields.shape, F32),
            (diffusivity.shape, F32),
            ((lines, LANE), jnp.int32),
            table,
            table,
            ((6 * count, LANE), F32),
            ((groups - 2, parts, width, ny), F32),
            ((2, parts, groups - 2, SUB, ny), F32),
        ],
        (fields, diffusivity, offsets, coupling, inverse),
        scratch=[pltpu.SemaphoreType.DMA(((parts + 1) * chunks,))],
        specs=[anywhere, anywhere, pl.BlockSpec(memory_space=pltpu.SMEM), vmem_spec(), vmem_spec()],
    )
    element_shape = ((2 * rows + 4 * count, half), F32)
    saved_shape = ((rows + 2 * count, half), F32)
    outer, send, mine = call(
        edge_kernel,
        [((2, parts, width, ny), F32), element_shape, element_shape],
        (fields_v, diff_v, west, east, offsb, k_rows, coefs, sides),
        scratch=[pltpu.VMEM((2, parts, 2, SUB, ny), F32)],
    )
    got = swap(send, 0)
    saved = []
    for bit in range(bits - 1):
        if bit < bits - 2:
            mine, kept = call(
                functools.partial(merge_kernel, bit, parts, count),
                [element_shape, saved_shape],
                (mine, got, offsb),
            )
            got = swap(mine, bit + 1)
        if bit == 0:
            solved, token = call(
                block_kernel,
                [((groups, parts, width, ny), F32), ((SUB, LANE), F32)],
                (mine, inner, outer, offsb, inverse),
                scratch=[
                    pltpu.VMEM((count, levels, width), F32),
                    pltpu.VMEM((groups, 2, width, width), BF16),
                ],
            )
        if bit == bits - 2:
            mine, kept, send = call(
                functools.partial(merge_last_kernel, bit, parts, count),
                [element_shape, saved_shape, ((rows + count, half), F32)],
                (mine, got, offsb, token),
            )
            got = swap(send, bit + 1)
        saved.append(kept)
    pair = ((2 * rows, half), F32)
    theirs, own = call(
        functools.partial(solve_kernel, bits - 1, parts, count),
        [pair, pair],
        (send, got, mine, offsb, *saved),
    )
    other = swap(theirs, 0)
    (out,) = call(
        functools.partial(finish_kernel, SUB),
        [((parts, levels, lines, ny), F32)],
        (solved, own, other, offsb, spikes),
        scratch=[pltpu.VMEM((parts, levels, lines, ny), F32), pltpu.SemaphoreType.DMA((parts * chunks,))],
        keep=False,
    )
    return out


def solution(mesh):
    return jax.shard_map(
        body,
        mesh=mesh,
        in_specs=(
            P(None, "depth", "horiz", None),
            P("depth", "horiz", None),
            P("horiz"),
            P(None, "depth"),
            P(None, "depth", None),
        ),
        out_specs=P(None, "depth", "horiz", None),
        check_vma=False,
    )
```

```python
import functools

import jax
import jax.numpy as jnp
from jax import lax
from jax.experimental import pallas as pl
from jax.experimental.pallas import tpu as pltpu
from jax.sharding import PartitionSpec as P

wave_gain = 0.5
SUB = 8
LANE = 128
VMEM = pltpu.VMEM
F32 = jnp.float32
BF16 = jnp.bfloat16


def vmem_spec():
    return pl.BlockSpec(memory_space=VMEM)


def choose(offs, rows):
    value = jnp.broadcast_to(rows[0], offs.shape)
    for o in range(1, len(rows)):
        value = jnp.where(offs == o, jnp.broadcast_to(rows[o], offs.shape), value)
    return value


def split_bf16(x):
    high = x.astype(BF16)
    low = (x - high.astype(F32)).astype(BF16)
    return high, low


def outermost_kernel(
    fields_ref,
    diff_ref,
    offs_hbm,
    coupling_hbm,
    inverse_hbm,
    side_ref,
    far_ref,
    diff_rows_ref,
    offs_ref,
    coupling_ref,
    inverse_ref,
    stage_ref,
    diff_stage_ref,
    sems,
):
    parts, levels, lines, ny = fields_ref.shape
    even = lax.axis_index("horiz") % 2 == 0
    copies = []
    for e, line in enumerate((0, lines - 1)):
        copy = pltpu.make_async_copy(fields_ref.at[:, :, pl.ds(line, 1), :], stage_ref.at[e], sems.at[e])
        copy.start()
        copies.append(copy)
        copy = pltpu.make_async_copy(diff_ref.at[:, pl.ds(line, 1), :], diff_stage_ref.at[e], sems.at[5 + e])
        copy.start()
        copies.append(copy)
    small = ((offs_hbm, offs_ref), (coupling_hbm, coupling_ref), (inverse_hbm, inverse_ref))
    for n, (source, target) in enumerate(small):
        copy = pltpu.make_async_copy(source, target, sems.at[2 + n])
        copy.start()
        copies.append(copy)
    for copy in copies:
        copy.wait()
    for i in range(parts):
        for c in range(levels // SUB):
            at = slice(c * SUB, (c + 1) * SUB)
            first, last = [gather_rows(lambda k: stage_ref[e, i, k, 0:1, :], c, ny) for e in range(2)]
            side_ref[i, at, :] = jnp.where(even, last, first)
            far_ref[i, at, :] = jnp.where(even, first, last)
    for e in range(2):
        for c in range(levels // SUB):
            diff_rows_ref[e, c * SUB : (c + 1) * SUB, :] = gather_rows(
                lambda k: diff_stage_ref[e, k, 0:1, :], c, ny
            )


def gather_rows(row_at, c, ny):
    sub = lax.broadcasted_iota(jnp.int32, (SUB, ny), 0)
    value = jnp.zeros((SUB, ny), F32)
    for t in range(SUB):
        value = jnp.where(sub == t, jnp.broadcast_to(row_at(c * SUB + t), value.shape), value)
    return value


def fill_tables(offs_ref, coupling_ref, inverse_ref, offsb_ref, spikes_ref, rows_ref, coefs_ref):
    count, levels, _ = inverse_ref.shape
    lines = offsb_ref.shape[0]
    rank = lax.axis_index("depth")

    square = (lines, lines)
    own = lax.broadcasted_iota(jnp.int32, square, 0) == lax.broadcasted_iota(jnp.int32, square, 1)
    row = jnp.broadcast_to(offs_ref[...].astype(F32), square)
    column = jnp.sum(jnp.where(own, row, jnp.zeros_like(row)), axis=1, keepdims=True)
    offsb_ref[...] = jnp.broadcast_to(column, (lines, LANE)).astype(jnp.int32)

    eye = lax.broadcasted_iota(jnp.int32, (levels, levels), 0) == lax.broadcasted_iota(
        jnp.int32, (levels, levels), 1
    )
    for o in range(count):
        gate = jnp.broadcast_to(coupling_ref[o : o + 1, levels - 1 : levels], (1, LANE))
        face = jnp.broadcast_to(coupling_ref[o : o + 1, 0:1], (1, LANE))
        face = jnp.where(rank > 0, face, jnp.zeros_like(face))
        low = jnp.broadcast_to(inverse_ref[o, :, 0:1], (levels, LANE)) * face
        high = jnp.broadcast_to(inverse_ref[o, :, levels - 2 : levels - 1], (levels, LANE)) * gate
        spikes_ref[0, o] = low
        spikes_ref[1, o] = high
        for k, level in enumerate((0, levels - 2)):
            row = jnp.broadcast_to(inverse_ref[o, level : level + 1, :], (levels, levels))
            column = jnp.sum(jnp.where(eye, row, jnp.zeros_like(row)), axis=1, keepdims=True)
            rows_ref[k, o] = jnp.broadcast_to(column, (levels, LANE))
        b = face - face * low[0:1]
        e = -face * high[0:1]
        l = -gate * low[levels - 2 : levels - 1]
        a = 1.0 + gate - gate * high[levels - 2 : levels - 1]
        for c, row in enumerate((b, e, l, a, gate, face)):
            coefs_ref[c * count + o : c * count + o + 1, :] = row


def force_group(g, fields_ref, diff_ref, offsb_ref, rows_ref, coefs_ref, forcing_ref, sides_ref):
    parts, levels, lines, ny = fields_ref.shape
    groups = lines // SUB
    half = ny // 2
    count = rows_ref.shape[1]
    first = g * SUB
    sub = lax.broadcasted_iota(jnp.int32, (SUB, ny), 0)
    offs = offsb_ref[first : first + SUB, :]
    gate = choose(offs, [coefs_ref[4 * count + o : 4 * count + o + 1, :] for o in range(count)])
    face = choose(offs, [coefs_ref[5 * count + o : 5 * count + o + 1, :] for o in range(count)])

    def one_level(k, sums):
        centre, across, along, both = [], [], [], []
        for i in range(parts):
            c = fields_ref[i, k, first : first + SUB, :]
            north = pltpu.roll(c, ny - 1, 1)
            south = pltpu.roll(c, 1, 1)
            if g > 0:
                row_w = fields_ref[i, k, first - 1 : first, :]
            else:
                row_w = jnp.zeros((1, ny), F32)
            if g < groups - 1:
                row_e = fields_ref[i, k, first + SUB : first + SUB + 1, :]
            else:
                row_e = jnp.zeros((1, ny), F32)
            east = jnp.where(sub == SUB - 1, jnp.broadcast_to(row_e, c.shape), pltpu.roll(c, SUB - 1, 0))
            west = jnp.where(sub == 0, jnp.broadcast_to(row_w, c.shape), pltpu.roll(c, 1, 0))
            centre.append(c)
            both.append((east + west) + (north + south) - 4.0 * c)
            along.append(east - west)
            across.append(north - south)
        d = diff_ref[k, first : first + SUB, :]
        scale = 0.5 * wave_gain
        out = (
            centre[0] + d * both[0] - scale * along[2],
            centre[1] + d * both[1] - scale * across[2],
            centre[2] + d * both[2] - scale * (along[0] + across[1]),
        )
        at = pl.multiple_of(k * SUB, SUB)
        top = choose(offs, [rows_ref[0, o, pl.ds(k, 1), :] for o in range(count)])
        bottom = choose(offs, [rows_ref[1, o, pl.ds(k, 1), :] for o in range(count)])
        new = []
        for i in range(parts):
            forcing_ref[g, i, pl.ds(at, SUB), :] = out[i]
            for h in range(2):
                piece = out[i][:, h * half : (h + 1) * half]
                at_0, at_1 = sums[2 * (i * 2 + h)], sums[2 * (i * 2 + h) + 1]
                new += [at_0 + top * piece, at_1 + bottom * piece]
        return tuple(new)

    def close(sums):
        for i in range(parts):
            for h in range(2):
                cut = slice(h * half, (h + 1) * half)
                last = forcing_ref[g, i, (levels - 1) * SUB :, cut]
                at = i * lines + first
                sides_ref[at : at + SUB, cut] = last + gate * sums[2 * (i * 2 + h) + 1]
                at += parts * lines
                sides_ref[at : at + SUB, cut] = face * sums[2 * (i * 2 + h)]

    return one_level, tuple(jnp.zeros((SUB, half), F32) for _ in range(4 * parts)), close


def run_groups(groups, levels):
    for one_level, sums, close in groups:
        close(lax.fori_loop(0, levels, one_level, sums, unroll=SUB))


def inner_kernel(
    fields_ref,
    diff_ref,
    offs_ref,
    coupling_ref,
    inverse_ref,
    offsb_ref,
    spikes_ref,
    rows_ref,
    coefs_ref,
    forcing_ref,
    sides_ref,
):
    levels, lines, _ = diff_ref.shape
    fill_tables(offs_ref, coupling_ref, inverse_ref, offsb_ref, spikes_ref, rows_ref, coefs_ref)
    work = [
        force_group(g, fields_ref, diff_ref, offsb_ref, rows_ref, coefs_ref, forcing_ref, sides_ref)
        for g in range(lines // SUB)
    ]
    run_groups(work, levels)


def correct_kernel(
    side_ref, far_ref, sides_ref, diff_rows_ref, offsb_ref, rows_ref, coefs_ref, extra_ref, send_ref, keep_ref
):
    parts, levels, ny = side_ref.shape
    lines = offsb_ref.shape[0]
    half = ny // 2
    count = rows_ref.shape[1]
    core = lax.axis_index("depth") % 2
    even = lax.axis_index("horiz") % 2 == 0
    sub = lax.broadcasted_iota(jnp.int32, (SUB, half), 0)
    scale = 0.5 * wave_gain
    base = 2 * parts * lines
    for at in range(0, base, SUB):
        left, right = sides_ref[at : at + SUB, :half], sides_ref[at : at + SUB, half:]
        keep_ref[at : at + SUB, :] = jnp.where(core == 0, left, right)
        send_ref[at : at + SUB, :] = jnp.where(core == 0, right, left)
    send_ref[base : base + 4 * count, :] = coefs_ref[: 4 * count, :]
    keep_ref[base : base + 4 * count, :] = coefs_ref[: 4 * count, :]

    for e, (line, sign) in enumerate(((0, scale), (lines - 1, -scale))):
        near, other = (far_ref, side_ref) if e == 0 else (side_ref, far_ref)
        halo = [jnp.where(even, near[i], other[i]) for i in range(parts)]
        d = diff_rows_ref[e]
        extra = (d * halo[0] + sign * halo[2], d * halo[1], d * halo[2] + sign * halo[0])
        offs = jnp.broadcast_to(offsb_ref[line : line + 1, :], (levels, half))
        one = offs[:1]
        gate = choose(one, [coefs_ref[4 * count + o : 4 * count + o + 1, :] for o in range(count)])
        face = choose(one, [coefs_ref[5 * count + o : 5 * count + o + 1, :] for o in range(count)])
        top = choose(offs, [rows_ref[0, o] for o in range(count)])
        bottom = choose(offs, [rows_ref[1, o] for o in range(count)])
        group, place = line // SUB * SUB, line % SUB
        for i in range(parts):
            extra_ref[e, i] = extra[i]
            more = []
            for h in range(2):
                piece = extra[i][:, h * half : (h + 1) * half]
                a_side = piece[levels - 1 :, :] + gate * jnp.sum(bottom * piece, axis=0, keepdims=True)
                more.append((a_side, face * jnp.sum(top * piece, axis=0, keepdims=True)))
            for k in range(2):
                left, right = more[0][k], more[1][k]
                at = (k * parts + i) * lines + group
                zero = jnp.zeros((SUB, half), F32)
                for ref, row in (
                    (keep_ref, jnp.where(core == 0, left, right)),
                    (send_ref, jnp.where(core == 0, right, left)),
                ):
                    ref[at : at + SUB, :] += jnp.where(sub == place, jnp.broadcast_to(row, zero.shape), zero)


def block_kernel(
    after_ref, forcing_ref, extra_ref, offsb_ref, inverse_ref, solved_ref, token_ref, wide_ref, big_ref, work_ref
):
    count, levels, _ = inverse_ref.shape
    groups, parts, width, ny = solved_ref.shape
    token_ref[...] = after_ref[:SUB, :]

    spread = (
        lax.broadcasted_iota(jnp.int32, (levels, width), 1) // SUB
        == lax.broadcasted_iota(jnp.int32, (levels, width), 0)
    ).astype(F32)
    for o in range(count):
        wide_ref[o] = lax.dot_general(
            inverse_ref[o],
            spread,
            (((1,), (0,)), ((), ())),
            precision=lax.Precision.HIGHEST,
            preferred_element_type=F32,
        )
    lane = lax.broadcasted_iota(jnp.int32, (SUB, width), 1)
    sub = lax.broadcasted_iota(jnp.int32, (SUB, width), 0)
    diagonal = lane % SUB == sub
    zero = jnp.zeros((SUB, width), F32)
    offs_wide = [
        jnp.concatenate([offsb_ref[g * SUB : (g + 1) * SUB, :]] * (width // LANE), axis=1) for g in range(groups)
    ]

    def one_pair(k, _):
        rows = [[wide_ref[o, pl.ds(2 * k + i, 1), :] for o in range(count)] for i in range(2)]
        for g in range(groups):
            both = jnp.concatenate(
                [jnp.where(diagonal, choose(offs_wide[g], rows[i]), zero) for i in range(2)], axis=0
            )
            high, low = split_bf16(both)
            at = pl.multiple_of(k * 2 * SUB, 2 * SUB)
            big_ref[g, 0, pl.ds(at, 2 * SUB), :] = high
            big_ref[g, 1, pl.ds(at, 2 * SUB), :] = low
        return 0

    lax.fori_loop(0, levels // 2, one_pair, 0)
    here = lax.broadcasted_iota(jnp.int32, (SUB, ny), 0)
    nought = jnp.zeros((SUB, ny), F32)
    for g in range(groups):
        m_high = big_ref[g, 0]
        m_low = big_ref[g, 1]
        for i in range(parts):
            if 0 < g < groups - 1:
                x = forcing_ref[g, i]
            else:
                e, line = (0, 0) if g == 0 else (1, SUB - 1)
                for k in range(levels):
                    at = slice(k * SUB, (k + 1) * SUB)
                    row = jnp.broadcast_to(extra_ref[e, i, k : k + 1, :], (SUB, ny))
                    work_ref[e, i, at, :] = forcing_ref[g, i, at, :] + jnp.where(here == line, row, nought)
                x = work_ref[e, i]
            x_high, x_low = split_bf16(x)
            solved_ref[g, i] = (
                jnp.dot(m_high, x_high, preferred_element_type=F32)
                + jnp.dot(m_low, x_high, preferred_element_type=F32)
                + jnp.dot(m_high, x_low, preferred_element_type=F32)
            )


def unpack(ref, rows, count):
    a_side = ref[:rows, :]
    b_side = ref[rows : 2 * rows, :]
    base = 2 * rows
    b, e, l, a = [ref[base + c * count : base + (c + 1) * count, :] for c in range(4)]
    return a_side, b_side, b, e, l, a


def per_line(offs, table, parts):
    rows = [table[o : o + 1, :] for o in range(table.shape[0])]
    value = choose(offs, rows)
    return jnp.concatenate([value] * parts, axis=0)


def merged(bit, mine_ref, got_ref, offs, parts, count):
    lines = offs.shape[0]
    rows = parts * lines
    lower_is_mine = (lax.axis_index("depth") >> bit) % 2 == 0
    mine = unpack(mine_ref, rows, count)
    got = unpack(got_ref, rows, count)
    a_1, b_1, cb_1, ce_1, cl_1, ca_1 = [jnp.where(lower_is_mine, x, y) for x, y in zip(mine, got)]
    a_2, b_2, cb_2, ce_2, cl_2, ca_2 = [jnp.where(lower_is_mine, y, x) for x, y in zip(mine, got)]
    inverse = 1.0 / (ca_1 + cb_2)
    total = a_1 + b_2
    down = ce_1 * inverse
    up = cl_2 * inverse
    a_new = a_2 - per_line(offs, up, parts) * total
    b_new = b_1 - per_line(offs, down, parts) * total
    cb = cb_1 - down * cl_1
    ce = -down * ce_2
    cl = -up * cl_1
    ca = ca_2 - up * ce_2
    middle = per_line(offs, inverse, parts) * total
    return (a_new, b_new, cb, ce, cl, ca), (middle, cl_1 * inverse, ce_2 * inverse)


def store_saved(saved_ref, saved, count):
    middle, low, high = saved
    rows = middle.shape[0]
    saved_ref[:rows, :] = middle
    saved_ref[rows : rows + count, :] = low
    saved_ref[rows + count : rows + 2 * count, :] = high


def store_element(ref, element, count):
    rows = element[0].shape[0]
    ref[:rows, :] = element[0]
    ref[rows : 2 * rows, :] = element[1]
    for c in range(4):
        ref[2 * rows + c * count : 2 * rows + (c + 1) * count, :] = element[2 + c]


def merge_kernel(bit, parts, count, mine_ref, got_ref, offsb_ref, element_ref, saved_ref):
    element, saved = merged(bit, mine_ref, got_ref, offsb_ref[...], parts, count)
    store_element(element_ref, element, count)
    store_saved(saved_ref, saved, count)


def merge_last_kernel(bit, parts, count, mine_ref, got_ref, offsb_ref, token_ref, element_ref, saved_ref, send_ref):
    offs = offsb_ref[...]
    element, saved = merged(bit, mine_ref, got_ref, offs, parts, count)
    store_element(element_ref, element, count)
    store_saved(saved_ref, saved, count)
    a_side, b_side, cb, ce, cl, ca = element
    rows = a_side.shape[0]
    lower = (lax.axis_index("depth") >> (bit + 1)) == 0
    ratio = ce / ca
    send_ref[:rows, :] = jnp.where(lower, a_side, b_side - per_line(offs, ratio, parts) * a_side)
    send_ref[rows : rows + count, :] = jnp.where(lower, ca, cb - ratio * cl)


def solve_kernel(bits, parts, count, *refs):
    sent_ref, got_ref, element_ref, offsb_ref = refs[:4]
    saved_refs = refs[4 : 4 + bits]
    send_ref, keep_ref = refs[4 + bits :]
    offs = offsb_ref[...]
    rows = parts * offs.shape[0]
    rank = lax.axis_index("depth")
    pivot = sent_ref[rows : rows + count, :] + got_ref[rows : rows + count, :]
    shared = (sent_ref[:rows, :] + got_ref[:rows, :]) * per_line(offs, 1.0 / pivot, parts)
    a_side, _, _, _, cl, ca = unpack(element_ref, rows, count)
    inverse = 1.0 / ca
    top = per_line(offs, inverse, parts) * a_side - per_line(offs, cl * inverse, parts) * shared
    lower = (rank >> bits) == 0
    below = jnp.where(lower, jnp.zeros_like(shared), shared)
    above = jnp.where(lower, shared, top)
    for bit in reversed(range(bits)):
        saved_ref = saved_refs[bit]
        low = saved_ref[rows : rows + count, :]
        high = saved_ref[rows + count : rows + 2 * count, :]
        middle = saved_ref[:rows, :] - per_line(offs, low, parts) * below - per_line(offs, high, parts) * above
        lower = (rank >> bit) % 2 == 0
        if bit > 0:
            below, above = jnp.where(lower, below, middle), jnp.where(lower, middle, above)
        else:
            keep_ref[:rows, :] = jnp.where(lower, below, middle)
            keep_ref[rows:, :] = jnp.where(lower, middle, above)
            send_ref[:rows, :] = jnp.where(lower, middle, below)
            send_ref[rows:, :] = jnp.where(lower, above, middle)


def finish_kernel(step, own, solved_ref, ends_ref, offsb_ref, spikes_ref, *refs):
    out_ref, stage_ref, sems = refs[-3:]
    parts, levels, lines, ny = out_ref.shape
    groups = lines // SUB
    half = ny // 2
    count = spikes_ref.shape[1]
    rows = parts * lines
    core = lax.axis_index("depth") % 2
    cut = pl.ds(pl.multiple_of((core if own else 1 - core) * half, half), half)

    copies = []
    for c in range(levels // step):
        for g in range(groups):
            lane = slice(g * SUB, (g + 1) * SUB)
            offs = offsb_ref[lane, :]
            side = [
                [ends_ref[k * rows + i * lines + g * SUB : k * rows + i * lines + (g + 1) * SUB, :] for i in range(parts)]
                for k in range(2)
            ]
            for k in range(c * step, (c + 1) * step):
                if k == levels - 1:
                    for i in range(parts):
                        stage_ref[i, k, lane, :] = side[1][i]
                    continue
                low = choose(offs, [spikes_ref[0, o, k : k + 1, :] for o in range(count)])
                high = choose(offs, [spikes_ref[1, o, k : k + 1, :] for o in range(count)])
                for i in range(parts):
                    value = solved_ref[g, i, k * SUB : (k + 1) * SUB, cut]
                    stage_ref[i, k, lane, :] = value + low * side[0][i] + high * side[1][i]
        for i in range(parts):
            at = pl.ds(c * step, step)
            copy = pltpu.make_async_copy(stage_ref.at[i, at], out_ref.at[i, at, :, cut], sems.at[c * parts + i])
            copy.start()
            copies.append(copy)
    for copy in copies:
        copy.wait()


def call(kernel, outs, args, scratch=(), specs=None, **options):
    put = [pltpu.with_memory_space_constraint(x, VMEM) for x in args] if specs is None else args
    return pl.pallas_call(
        kernel,
        out_shape=[VMEM(s, d) for s, d in outs],
        in_specs=specs or [vmem_spec()] * len(args),
        out_specs=[vmem_spec()] * len(outs),
        scratch_shapes=list(scratch),
        compiler_params=pltpu.CompilerParams(vmem_limit_bytes=16 * 2**20),
    )(*put)


def finish(own, out_shape, args, before=None):
    step = SUB
    parts, levels, lines, ny = out_shape
    put = [pltpu.with_memory_space_constraint(x, VMEM) for x in args]
    specs = [vmem_spec()] * len(args)
    aliases = {}
    if before is not None:
        put.append(pltpu.with_memory_space_constraint(before, pltpu.HBM))
        specs.append(pl.BlockSpec(memory_space=pltpu.HBM))
        aliases = {len(args): 0}
    return pl.pallas_call(
        functools.partial(finish_kernel, step, own),
        out_shape=pltpu.HBM(out_shape, F32),
        in_specs=specs,
        out_specs=pl.BlockSpec(memory_space=pltpu.HBM),
        scratch_shapes=[
            pltpu.VMEM((parts, levels, lines, ny // 2), F32),
            pltpu.SemaphoreType.DMA((parts * (levels // step),)),
        ],
        input_output_aliases=aliases,
        compiler_params=pltpu.CompilerParams(vmem_limit_bytes=16 * 2**20),
    )(*put)


def body(fields, diffusivity, offsets, coupling, inverse):
    parts, levels, lines, ny = fields.shape
    count = inverse.shape[0]
    half = ny // 2
    groups = lines // SUB
    width = levels * SUB
    around = lax.axis_size("horiz")
    ranks = lax.axis_size("depth")
    bits = ranks.bit_length() - 1
    assert ranks == 1 << bits and bits >= 2 and around % 2 == 0 and half == LANE and groups >= 2

    def swap(x, bit):
        return lax.ppermute(x, "depth", [(i, i ^ (1 << bit)) for i in range(ranks)])

    in_hbm = pl.BlockSpec(memory_space=pltpu.HBM)
    edge = ((parts, levels, ny), F32)
    offsets = offsets.reshape(1, lines)
    to_side, to_far, diff_rows, offsets, coupling, inverse = call(
        outermost_kernel,
        [edge, edge, ((2, levels, ny), F32), (offsets.shape, jnp.int32), (coupling.shape, F32), (inverse.shape, F32)],
        [pltpu.with_memory_space_constraint(x, pltpu.HBM) for x in (fields, diffusivity, offsets, coupling, inverse)],
        scratch=[
            pltpu.VMEM((2, parts, levels, 1, ny), F32),
            pltpu.VMEM((2, levels, 1, ny), F32),
            pltpu.SemaphoreType.DMA((7,)),
        ],
        specs=[in_hbm] * 5,
    )
    far = lax.ppermute(to_far, "horiz", [(i, (i + 2 * (i % 2) - 1) % around) for i in range(around)])
    side = lax.ppermute(to_side, "horiz", [(i, (i + 1 - 2 * (i % 2)) % around) for i in range(around)])

    rows = parts * lines
    table = ((2, count, levels, LANE), F32)
    offsb, spikes, k_rows, coefs, forcing, sides = call(
        inner_kernel,
        [
            ((lines, LANE), jnp.int32),
            table,
            table,
            ((6 * count, LANE), F32),
            ((groups, parts, width, ny), F32),
            ((2 * rows, ny), F32),
        ],
        (fields, diffusivity, offsets, coupling, inverse),
        specs=[vmem_spec()] * 5,
    )
    element_shape = ((2 * rows + 4 * count, half), F32)
    saved_shape = ((rows + 2 * count, half), F32)
    extra, send, mine = call(
        correct_kernel,
        [((2, parts, levels, ny), F32), element_shape, element_shape],
        (side, far, sides, diff_rows, offsb, k_rows, coefs),
    )
    got = swap(send, 0)
    saved = []
    for bit in range(bits - 1):
        if bit < bits - 2:
            mine, kept = call(
                functools.partial(merge_kernel, bit, parts, count),
                [element_shape, saved_shape],
                (mine, got, offsb),
            )
            got = swap(mine, bit + 1)
        if bit == 0:
            solved, token = call(
                block_kernel,
                [((groups, parts, width, ny), F32), ((SUB, LANE), F32)],
                (mine, forcing, extra, offsb, inverse),
                scratch=[
                    pltpu.VMEM((count, levels, width), F32),
                    pltpu.VMEM((groups, 2, width, width), BF16),
                    pltpu.VMEM((2, parts, width, ny), F32),
                ],
            )
        if bit == bits - 2:
            mine, kept, send = call(
                functools.partial(merge_last_kernel, bit, parts, count),
                [element_shape, saved_shape, ((rows + count, half), F32)],
                (mine, got, offsb, token),
            )
            got = swap(send, bit + 1)
        saved.append(kept)
    pair = ((2 * rows, half), F32)
    theirs, own = call(
        functools.partial(solve_kernel, bits - 1, parts, count),
        [pair, pair],
        (send, got, mine, offsb, *saved),
    )
    other = swap(theirs, 0)
    half_out = finish(True, (parts, levels, lines, ny), (solved, own, offsb, spikes))
    return finish(False, (parts, levels, lines, ny), (solved, other, offsb, spikes), half_out)


def solution(mesh):
    return jax.shard_map(
        body,
        mesh=mesh,
        in_specs=(
            P(None, "depth", "horiz", None),
            P("depth", "horiz", None),
            P("horiz"),
            P(None, "depth"),
            P(None, "depth", None),
        ),
        out_specs=P(None, "depth", "horiz", None),
        check_vma=False,
    )
```

```python
import functools

import jax
import jax.numpy as jnp
from jax import lax
from jax.experimental import pallas as pl
from jax.experimental.pallas import tpu as pltpu
from jax.sharding import PartitionSpec as P

wave_gain = 0.5
SUB = 8
LANE = 128
VMEM = pltpu.VMEM
F32 = jnp.float32
BF16 = jnp.bfloat16


def vmem_spec():
    return pl.BlockSpec(memory_space=VMEM)


def choose(offs, rows):
    value = jnp.broadcast_to(rows[0], offs.shape)
    for o in range(1, len(rows)):
        value = jnp.where(offs == o, jnp.broadcast_to(rows[o], offs.shape), value)
    return value


def split_bf16(x):
    high = x.astype(BF16)
    low = (x - high.astype(F32)).astype(BF16)
    return high, low


def outermost_kernel(
    fields_ref,
    diff_ref,
    offs_hbm,
    coupling_hbm,
    inverse_hbm,
    side_ref,
    far_ref,
    diff_stage_ref,
    offs_ref,
    coupling_ref,
    inverse_ref,
    stage_ref,
    sems,
):
    parts, levels, lines, ny = fields_ref.shape
    even = lax.axis_index("horiz") % 2 == 0
    copies = []
    for e, line in enumerate((0, lines - 1)):
        copy = pltpu.make_async_copy(fields_ref.at[:, :, pl.ds(line, 1), :], stage_ref.at[e], sems.at[e])
        copy.start()
        copies.append(copy)
        copy = pltpu.make_async_copy(diff_ref.at[:, pl.ds(line, 1), :], diff_stage_ref.at[e], sems.at[5 + e])
        copy.start()
        copies.append(copy)
    small = ((offs_hbm, offs_ref), (coupling_hbm, coupling_ref), (inverse_hbm, inverse_ref))
    for n, (source, target) in enumerate(small):
        copy = pltpu.make_async_copy(source, target, sems.at[2 + n])
        copy.start()
        copies.append(copy)
    for copy in copies:
        copy.wait()
    for i in range(parts):
        for c in range(levels // SUB):
            at = slice(c * SUB, (c + 1) * SUB)
            first, last = [gather_rows(lambda k: stage_ref[e, i, k, 0:1, :], c, ny) for e in range(2)]
            side_ref[i, at, :] = jnp.where(even, last, first)
            far_ref[i, at, :] = jnp.where(even, first, last)


def gather_rows(row_at, c, ny):
    sub = lax.broadcasted_iota(jnp.int32, (SUB, ny), 0)
    value = jnp.broadcast_to(row_at(c * SUB), (SUB, ny))
    for t in range(1, SUB):
        value = jnp.where(sub == t, jnp.broadcast_to(row_at(c * SUB + t), value.shape), value)
    return value


def fill_tables(offs_ref, coupling_ref, inverse_ref, offsb_ref, spikes_ref, rows_ref, coefs_ref):
    count, levels, _ = inverse_ref.shape
    lines = offsb_ref.shape[0]
    rank = lax.axis_index("depth")

    square = (lines, lines)
    own = lax.broadcasted_iota(jnp.int32, square, 0) == lax.broadcasted_iota(jnp.int32, square, 1)
    row = jnp.broadcast_to(offs_ref[...].astype(F32), square)
    column = jnp.sum(jnp.where(own, row, jnp.zeros_like(row)), axis=1, keepdims=True)
    offsb_ref[...] = jnp.broadcast_to(column, (lines, LANE)).astype(jnp.int32)

    eye = lax.broadcasted_iota(jnp.int32, (levels, levels), 0) == lax.broadcasted_iota(
        jnp.int32, (levels, levels), 1
    )
    for o in range(count):
        gate = jnp.broadcast_to(coupling_ref[o : o + 1, levels - 1 : levels], (1, LANE))
        face = jnp.broadcast_to(coupling_ref[o : o + 1, 0:1], (1, LANE))
        face = jnp.where(rank > 0, face, jnp.zeros_like(face))
        low = jnp.broadcast_to(inverse_ref[o, :, 0:1], (levels, LANE)) * face
        high = jnp.broadcast_to(inverse_ref[o, :, levels - 2 : levels - 1], (levels, LANE)) * gate
        spikes_ref[0, o] = low
        spikes_ref[1, o] = high
        for k, level in enumerate((0, levels - 2)):
            row = jnp.broadcast_to(inverse_ref[o, level : level + 1, :], (levels, levels))
            column = jnp.sum(jnp.where(eye, row, jnp.zeros_like(row)), axis=1, keepdims=True)
            rows_ref[k, o] = jnp.broadcast_to(column, (levels, LANE))
        b = face - face * low[0:1]
        e = -face * high[0:1]
        l = -gate * low[levels - 2 : levels - 1]
        a = 1.0 + gate - gate * high[levels - 2 : levels - 1]
        for c, row in enumerate((b, e, l, a, gate, face)):
            coefs_ref[c * count + o : c * count + o + 1, :] = row


def force_group(g, fields_ref, diff_ref, offsb_ref, rows_ref, coefs_ref, forcing_ref, sides_ref):
    parts, levels, lines, ny = fields_ref.shape
    groups = lines // SUB
    half = ny // 2
    count = rows_ref.shape[1]
    first = g * SUB
    sub = lax.broadcasted_iota(jnp.int32, (SUB, ny), 0)
    offs = offsb_ref[first : first + SUB, :]
    gate = choose(offs, [coefs_ref[4 * count + o : 4 * count + o + 1, :] for o in range(count)])
    face = choose(offs, [coefs_ref[5 * count + o : 5 * count + o + 1, :] for o in range(count)])

    def one_level(k, sums):
        centre, across, along, both = [], [], [], []
        for i in range(parts):
            c = fields_ref[i, k, first : first + SUB, :]
            north = pltpu.roll(c, ny - 1, 1)
            south = pltpu.roll(c, 1, 1)
            if g > 0:
                row_w = fields_ref[i, k, first - 1 : first, :]
            else:
                row_w = jnp.zeros((1, ny), F32)
            if g < groups - 1:
                row_e = fields_ref[i, k, first + SUB : first + SUB + 1, :]
            else:
                row_e = jnp.zeros((1, ny), F32)
            east = jnp.where(sub == SUB - 1, jnp.broadcast_to(row_e, c.shape), pltpu.roll(c, SUB - 1, 0))
            west = jnp.where(sub == 0, jnp.broadcast_to(row_w, c.shape), pltpu.roll(c, 1, 0))
            centre.append(c)
            both.append((east + west) + (north + south))
            along.append(east - west)
            across.append(north - south)
        d = diff_ref[k, first : first + SUB, :]
        rest = 1.0 - 4.0 * d
        scale = 0.5 * wave_gain
        out = (
            rest * centre[0] + d * both[0] - scale * along[2],
            rest * centre[1] + d * both[1] - scale * across[2],
            rest * centre[2] + d * both[2] - scale * (along[0] + across[1]),
        )
        at = pl.multiple_of(k * SUB, SUB)
        top = choose(offs, [rows_ref[0, o, pl.ds(k, 1), :] for o in range(count)])
        bottom = choose(offs, [rows_ref[1, o, pl.ds(k, 1), :] for o in range(count)])
        new = []
        for i in range(parts):
            forcing_ref[g, i, pl.ds(at, SUB), :] = out[i]
            for h in range(2):
                piece = out[i][:, h * half : (h + 1) * half]
                at_0, at_1 = sums[2 * (i * 2 + h)], sums[2 * (i * 2 + h) + 1]
                new += [at_0 + top * piece, at_1 + bottom * piece]
        return tuple(new)

    def close(sums):
        for i in range(parts):
            for h in range(2):
                cut = slice(h * half, (h + 1) * half)
                last = forcing_ref[g, i, (levels - 1) * SUB :, cut]
                at = i * lines + first
                sides_ref[at : at + SUB, cut] = last + gate * sums[2 * (i * 2 + h) + 1]
                at += parts * lines
                sides_ref[at : at + SUB, cut] = face * sums[2 * (i * 2 + h)]

    return one_level, tuple(jnp.zeros((SUB, half), F32) for _ in range(4 * parts)), close


def run_groups(groups, levels, waits):
    for n, (one_level, sums, close) in enumerate(groups):
        if n == 0:
            step = levels // len(waits)
            for c, wait in enumerate(waits):
                wait()
                sums = lax.fori_loop(c * step, (c + 1) * step, one_level, sums, unroll=True)
        else:
            sums = lax.fori_loop(0, levels, one_level, sums, unroll=True)
        close(sums)


def inner_kernel(
    fields_hbm,
    diff_hbm,
    diff_stage_ref,
    offs_ref,
    coupling_ref,
    inverse_ref,
    offsb_ref,
    spikes_ref,
    rows_ref,
    coefs_ref,
    forcing_ref,
    sides_ref,
    diff_rows_ref,
    fields_ref,
    diff_ref,
    sems,
):
    parts, levels, lines, ny = fields_ref.shape
    chunks = sems.shape[0] // (parts + 1)
    step = levels // chunks
    waits = []
    for c in range(chunks):
        at = pl.ds(c * step, step)
        pairs = [(fields_hbm.at[i, at], fields_ref.at[i, at]) for i in range(parts)]
        pairs.append((diff_hbm.at[at], diff_ref.at[at]))
        copies = [
            pltpu.make_async_copy(source, target, sems.at[c * (parts + 1) + n])
            for n, (source, target) in enumerate(pairs)
        ]
        for copy in copies:
            copy.start()
        waits.append(lambda copies=copies: [copy.wait() for copy in copies])
    fill_tables(offs_ref, coupling_ref, inverse_ref, offsb_ref, spikes_ref, rows_ref, coefs_ref)
    for e in range(2):
        for c in range(levels // SUB):
            diff_rows_ref[e, c * SUB : (c + 1) * SUB, :] = gather_rows(
                lambda k: diff_stage_ref[e, k, 0:1, :], c, ny
            )
    work = [
        force_group(g, fields_ref, diff_ref, offsb_ref, rows_ref, coefs_ref, forcing_ref, sides_ref)
        for g in range(lines // SUB)
    ]
    run_groups(work, levels, waits)


def correct_kernel(
    side_ref, far_ref, sides_ref, diff_rows_ref, offsb_ref, rows_ref, coefs_ref, extra_ref, send_ref, keep_ref
):
    parts, levels, ny = side_ref.shape
    lines = offsb_ref.shape[0]
    half = ny // 2
    count = rows_ref.shape[1]
    core = lax.axis_index("depth") % 2
    even = lax.axis_index("horiz") % 2 == 0
    sub = lax.broadcasted_iota(jnp.int32, (SUB, half), 0)
    scale = 0.5 * wave_gain
    base = 2 * parts * lines
    for at in range(0, base, SUB):
        left, right = sides_ref[at : at + SUB, :half], sides_ref[at : at + SUB, half:]
        keep_ref[at : at + SUB, :] = jnp.where(core == 0, left, right)
        send_ref[at : at + SUB, :] = jnp.where(core == 0, right, left)
    send_ref[base : base + 4 * count, :] = coefs_ref[: 4 * count, :]
    keep_ref[base : base + 4 * count, :] = coefs_ref[: 4 * count, :]

    for e, (line, sign) in enumerate(((0, scale), (lines - 1, -scale))):
        near, other = (far_ref, side_ref) if e == 0 else (side_ref, far_ref)
        halo = [jnp.where(even, near[i], other[i]) for i in range(parts)]
        d = diff_rows_ref[e]
        extra = (d * halo[0] + sign * halo[2], d * halo[1], d * halo[2] + sign * halo[0])
        offs = jnp.broadcast_to(offsb_ref[line : line + 1, :], (levels, half))
        one = offs[:1]
        gate = choose(one, [coefs_ref[4 * count + o : 4 * count + o + 1, :] for o in range(count)])
        face = choose(one, [coefs_ref[5 * count + o : 5 * count + o + 1, :] for o in range(count)])
        top = choose(offs, [rows_ref[0, o] for o in range(count)])
        bottom = choose(offs, [rows_ref[1, o] for o in range(count)])
        group, place = line // SUB * SUB, line % SUB
        for i in range(parts):
            extra_ref[e, i] = extra[i]
            more = []
            for h in range(2):
                piece = extra[i][:, h * half : (h + 1) * half]
                a_side = piece[levels - 1 :, :] + gate * jnp.sum(bottom * piece, axis=0, keepdims=True)
                more.append((a_side, face * jnp.sum(top * piece, axis=0, keepdims=True)))
            for k in range(2):
                left, right = more[0][k], more[1][k]
                at = (k * parts + i) * lines + group
                zero = jnp.zeros((SUB, half), F32)
                for ref, row in (
                    (keep_ref, jnp.where(core == 0, left, right)),
                    (send_ref, jnp.where(core == 0, right, left)),
                ):
                    ref[at : at + SUB, :] += jnp.where(sub == place, jnp.broadcast_to(row, zero.shape), zero)


def block_kernel(
    after_ref, forcing_ref, extra_ref, offsb_ref, inverse_ref, solved_ref, token_ref, wide_ref, big_ref, work_ref
):
    count, levels, _ = inverse_ref.shape
    groups, parts, width, ny = solved_ref.shape
    token_ref[...] = after_ref[:SUB, :]

    spread = (
        lax.broadcasted_iota(jnp.int32, (levels, width), 1) // SUB
        == lax.broadcasted_iota(jnp.int32, (levels, width), 0)
    ).astype(F32)
    for o in range(count):
        wide_ref[o] = lax.dot_general(
            inverse_ref[o],
            spread,
            (((1,), (0,)), ((), ())),
            precision=lax.Precision.HIGHEST,
            preferred_element_type=F32,
        )
    lane = lax.broadcasted_iota(jnp.int32, (SUB, width), 1)
    sub = lax.broadcasted_iota(jnp.int32, (SUB, width), 0)
    diagonal = lane % SUB == sub
    zero = jnp.zeros((SUB, width), F32)
    offs_wide = [
        jnp.concatenate([offsb_ref[g * SUB : (g + 1) * SUB, :]] * (width // LANE), axis=1) for g in range(groups)
    ]

    def one_pair(k, _):
        rows = [[wide_ref[o, pl.ds(2 * k + i, 1), :] for o in range(count)] for i in range(2)]
        for g in range(groups):
            both = jnp.concatenate(
                [jnp.where(diagonal, choose(offs_wide[g], rows[i]), zero) for i in range(2)], axis=0
            )
            high, low = split_bf16(both)
            at = pl.multiple_of(k * 2 * SUB, 2 * SUB)
            big_ref[g, 0, pl.ds(at, 2 * SUB), :] = high
            big_ref[g, 1, pl.ds(at, 2 * SUB), :] = low
        return 0

    lax.fori_loop(0, levels // 2, one_pair, 0)
    here = lax.broadcasted_iota(jnp.int32, (SUB, ny), 0)
    nought = jnp.zeros((SUB, ny), F32)
    for g in range(groups):
        m_high = big_ref[g, 0]
        m_low = big_ref[g, 1]
        for i in range(parts):
            if 0 < g < groups - 1:
                x = forcing_ref[g, i]
            else:
                e, line = (0, 0) if g == 0 else (1, SUB - 1)
                for k in range(levels):
                    at = slice(k * SUB, (k + 1) * SUB)
                    row = jnp.broadcast_to(extra_ref[e, i, k : k + 1, :], (SUB, ny))
                    work_ref[e, i, at, :] = forcing_ref[g, i, at, :] + jnp.where(here == line, row, nought)
                x = work_ref[e, i]
            x_high, x_low = split_bf16(x)
            solved_ref[g, i] = (
                jnp.dot(m_high, x_high, preferred_element_type=F32)
                + jnp.dot(m_low, x_high, preferred_element_type=F32)
                + jnp.dot(m_high, x_low, preferred_element_type=F32)
            )


def unpack(ref, rows, count):
    a_side = ref[:rows, :]
    b_side = ref[rows : 2 * rows, :]
    base = 2 * rows
    b, e, l, a = [ref[base + c * count : base + (c + 1) * count, :] for c in range(4)]
    return a_side, b_side, b, e, l, a


def per_line(offs, table, parts):
    rows = [table[o : o + 1, :] for o in range(table.shape[0])]
    value = choose(offs, rows)
    return jnp.concatenate([value] * parts, axis=0)


def merged(bit, mine_ref, got_ref, offs, parts, count):
    lines = offs.shape[0]
    rows = parts * lines
    lower_is_mine = (lax.axis_index("depth") >> bit) % 2 == 0
    mine = unpack(mine_ref, rows, count)
    got = unpack(got_ref, rows, count)
    a_1, b_1, cb_1, ce_1, cl_1, ca_1 = [jnp.where(lower_is_mine, x, y) for x, y in zip(mine, got)]
    a_2, b_2, cb_2, ce_2, cl_2, ca_2 = [jnp.where(lower_is_mine, y, x) for x, y in zip(mine, got)]
    inverse = 1.0 / (ca_1 + cb_2)
    total = a_1 + b_2
    down = ce_1 * inverse
    up = cl_2 * inverse
    a_new = a_2 - per_line(offs, up, parts) * total
    b_new = b_1 - per_line(offs, down, parts) * total
    cb = cb_1 - down * cl_1
    ce = -down * ce_2
    cl = -up * cl_1
    ca = ca_2 - up * ce_2
    middle = per_line(offs, inverse, parts) * total
    return (a_new, b_new, cb, ce, cl, ca), (middle, cl_1 * inverse, ce_2 * inverse)


def store_saved(saved_ref, saved, count):
    middle, low, high = saved
    rows = middle.shape[0]
    saved_ref[:rows, :] = middle
    saved_ref[rows : rows + count, :] = low
    saved_ref[rows + count : rows + 2 * count, :] = high


def store_element(ref, element, count):
    rows = element[0].shape[0]
    ref[:rows, :] = element[0]
    ref[rows : 2 * rows, :] = element[1]
    for c in range(4):
        ref[2 * rows + c * count : 2 * rows + (c + 1) * count, :] = element[2 + c]


def merge_kernel(bit, parts, count, mine_ref, got_ref, offsb_ref, element_ref, saved_ref):
    element, saved = merged(bit, mine_ref, got_ref, offsb_ref[...], parts, count)
    store_element(element_ref, element, count)
    store_saved(saved_ref, saved, count)


def merge_last_kernel(bit, parts, count, mine_ref, got_ref, offsb_ref, token_ref, element_ref, saved_ref, send_ref):
    offs = offsb_ref[...]
    element, saved = merged(bit, mine_ref, got_ref, offs, parts, count)
    store_element(element_ref, element, count)
    store_saved(saved_ref, saved, count)
    a_side, b_side, cb, ce, cl, ca = element
    rows = a_side.shape[0]
    lower = (lax.axis_index("depth") >> (bit + 1)) == 0
    ratio = ce / ca
    send_ref[:rows, :] = jnp.where(lower, a_side, b_side - per_line(offs, ratio, parts) * a_side)
    send_ref[rows : rows + count, :] = jnp.where(lower, ca, cb - ratio * cl)


def solve_kernel(bits, parts, count, *refs):
    sent_ref, got_ref, element_ref, offsb_ref = refs[:4]
    saved_refs = refs[4 : 4 + bits]
    send_ref, keep_ref = refs[4 + bits :]
    offs = offsb_ref[...]
    rows = parts * offs.shape[0]
    rank = lax.axis_index("depth")
    pivot = sent_ref[rows : rows + count, :] + got_ref[rows : rows + count, :]
    shared = (sent_ref[:rows, :] + got_ref[:rows, :]) * per_line(offs, 1.0 / pivot, parts)
    a_side, _, _, _, cl, ca = unpack(element_ref, rows, count)
    inverse = 1.0 / ca
    top = per_line(offs, inverse, parts) * a_side - per_line(offs, cl * inverse, parts) * shared
    lower = (rank >> bits) == 0
    below = jnp.where(lower, jnp.zeros_like(shared), shared)
    above = jnp.where(lower, shared, top)
    for bit in reversed(range(bits)):
        saved_ref = saved_refs[bit]
        low = saved_ref[rows : rows + count, :]
        high = saved_ref[rows + count : rows + 2 * count, :]
        middle = saved_ref[:rows, :] - per_line(offs, low, parts) * below - per_line(offs, high, parts) * above
        lower = (rank >> bit) % 2 == 0
        if bit > 0:
            below, above = jnp.where(lower, below, middle), jnp.where(lower, middle, above)
        else:
            keep_ref[:rows, :] = jnp.where(lower, below, middle)
            keep_ref[rows:, :] = jnp.where(lower, middle, above)
            send_ref[:rows, :] = jnp.where(lower, middle, below)
            send_ref[rows:, :] = jnp.where(lower, above, middle)


def finish_kernel(step, own, solved_ref, ends_ref, offsb_ref, spikes_ref, *refs):
    out_ref, stage_ref, sems = refs[-3:]
    parts, levels, lines, ny = out_ref.shape
    groups = lines // SUB
    half = ny // 2
    count = spikes_ref.shape[1]
    rows = parts * lines
    core = lax.axis_index("depth") % 2
    cut = pl.ds(pl.multiple_of((core if own else 1 - core) * half, half), half)

    copies = []
    for c in range(levels // step):
        for g in range(groups):
            lane = slice(g * SUB, (g + 1) * SUB)
            offs = offsb_ref[lane, :]
            side = [
                [ends_ref[k * rows + i * lines + g * SUB : k * rows + i * lines + (g + 1) * SUB, :] for i in range(parts)]
                for k in range(2)
            ]
            for k in range(c * step, (c + 1) * step):
                if k == levels - 1:
                    for i in range(parts):
                        stage_ref[i, k, lane, :] = side[1][i]
                    continue
                low = choose(offs, [spikes_ref[0, o, k : k + 1, :] for o in range(count)])
                high = choose(offs, [spikes_ref[1, o, k : k + 1, :] for o in range(count)])
                for i in range(parts):
                    value = solved_ref[g, i, k * SUB : (k + 1) * SUB, cut]
                    stage_ref[i, k, lane, :] = value + low * side[0][i] + high * side[1][i]
        for i in range(parts):
            at = pl.ds(c * step, step)
            copy = pltpu.make_async_copy(stage_ref.at[i, at], out_ref.at[i, at, :, cut], sems.at[c * parts + i])
            copy.start()
            copies.append(copy)
    for copy in copies:
        copy.wait()


def call(kernel, outs, args, scratch=(), specs=None, **options):
    put = [pltpu.with_memory_space_constraint(x, VMEM) for x in args] if specs is None else args
    return pl.pallas_call(
        kernel,
        out_shape=[VMEM(s, d) for s, d in outs],
        in_specs=specs or [vmem_spec()] * len(args),
        out_specs=[vmem_spec()] * len(outs),
        scratch_shapes=list(scratch),
        compiler_params=pltpu.CompilerParams(vmem_limit_bytes=16 * 2**20),
    )(*put)


def finish(own, out_shape, args, before=None):
    step = SUB
    parts, levels, lines, ny = out_shape
    put = [pltpu.with_memory_space_constraint(x, VMEM) for x in args]
    specs = [vmem_spec()] * len(args)
    aliases = {}
    if before is not None:
        put.append(pltpu.with_memory_space_constraint(before, pltpu.HBM))
        specs.append(pl.BlockSpec(memory_space=pltpu.HBM))
        aliases = {len(args): 0}
    return pl.pallas_call(
        functools.partial(finish_kernel, step, own),
        out_shape=pltpu.HBM(out_shape, F32),
        in_specs=specs,
        out_specs=pl.BlockSpec(memory_space=pltpu.HBM),
        scratch_shapes=[
            pltpu.VMEM((parts, levels, lines, ny // 2), F32),
            pltpu.SemaphoreType.DMA((parts * (levels // step),)),
        ],
        input_output_aliases=aliases,
        compiler_params=pltpu.CompilerParams(vmem_limit_bytes=16 * 2**20),
    )(*put)


def body(fields, diffusivity, offsets, coupling, inverse):
    parts, levels, lines, ny = fields.shape
    count = inverse.shape[0]
    half = ny // 2
    groups = lines // SUB
    width = levels * SUB
    around = lax.axis_size("horiz")
    ranks = lax.axis_size("depth")
    bits = ranks.bit_length() - 1
    assert ranks == 1 << bits and bits >= 2 and around % 2 == 0 and half == LANE and groups >= 2

    def swap(x, bit):
        return lax.ppermute(x, "depth", [(i, i ^ (1 << bit)) for i in range(ranks)])

    in_hbm = pl.BlockSpec(memory_space=pltpu.HBM)
    edge = ((parts, levels, ny), F32)
    offsets = offsets.reshape(1, lines)
    to_side, to_far, diff_stage, offsets, coupling, inverse = call(
        outermost_kernel,
        [edge, edge, ((2, levels, 1, ny), F32), (offsets.shape, jnp.int32), (coupling.shape, F32), (inverse.shape, F32)],
        [pltpu.with_memory_space_constraint(x, pltpu.HBM) for x in (fields, diffusivity, offsets, coupling, inverse)],
        scratch=[
            pltpu.VMEM((2, parts, levels, 1, ny), F32),
            pltpu.SemaphoreType.DMA((7,)),
        ],
        specs=[in_hbm] * 5,
    )
    far = lax.ppermute(to_far, "horiz", [(i, (i + 2 * (i % 2) - 1) % around) for i in range(around)])
    side = lax.ppermute(to_side, "horiz", [(i, (i + 1 - 2 * (i % 2)) % around) for i in range(around)])

    rows = parts * lines
    table = ((2, count, levels, LANE), F32)
    offsb, spikes, k_rows, coefs, forcing, sides, diff_rows = call(
        inner_kernel,
        [
            ((lines, LANE), jnp.int32),
            table,
            table,
            ((6 * count, LANE), F32),
            ((groups, parts, width, ny), F32),
            ((2 * rows, ny), F32),
            ((2, levels, ny), F32),
        ],
        [pltpu.with_memory_space_constraint(x, pltpu.HBM) for x in (fields, diffusivity)]
        + [diff_stage, offsets, coupling, inverse],
        scratch=[
            pltpu.VMEM(fields.shape, F32),
            pltpu.VMEM(diffusivity.shape, F32),
            pltpu.SemaphoreType.DMA(((parts + 1) * (levels // SUB),)),
        ],
        specs=[in_hbm] * 2 + [vmem_spec()] * 4,
    )
    element_shape = ((2 * rows + 4 * count, half), F32)
    saved_shape = ((rows + 2 * count, half), F32)
    extra, send, mine = call(
        correct_kernel,
        [((2, parts, levels, ny), F32), element_shape, element_shape],
        (side, far, sides, diff_rows, offsb, k_rows, coefs),
    )
    got = swap(send, 0)
    saved = []
    for bit in range(bits - 1):
        if bit < bits - 2:
            mine, kept = call(
                functools.partial(merge_kernel, bit, parts, count),
                [element_shape, saved_shape],
                (mine, got, offsb),
            )
            got = swap(mine, bit + 1)
        if bit == 0:
            solved, token = call(
                block_kernel,
                [((groups, parts, width, ny), F32), ((SUB, LANE), F32)],
                (mine, forcing, extra, offsb, inverse),
                scratch=[
                    pltpu.VMEM((count, levels, width), F32),
                    pltpu.VMEM((groups, 2, width, width), BF16),
                    pltpu.VMEM((2, parts, width, ny), F32),
                ],
            )
        if bit == bits - 2:
            mine, kept, send = call(
                functools.partial(merge_last_kernel, bit, parts, count),
                [element_shape, saved_shape, ((rows + count, half), F32)],
                (mine, got, offsb, token),
            )
            got = swap(send, bit + 1)
        saved.append(kept)
    pair = ((2 * rows, half), F32)
    theirs, own = call(
        functools.partial(solve_kernel, bits - 1, parts, count),
        [pair, pair],
        (send, got, mine, offsb, *saved),
    )
    other = swap(theirs, 0)
    half_out = finish(True, (parts, levels, lines, ny), (solved, own, offsb, spikes))
    return finish(False, (parts, levels, lines, ny), (solved, other, offsb, spikes), half_out)


def solution(mesh):
    return jax.shard_map(
        body,
        mesh=mesh,
        in_specs=(
            P(None, "depth", "horiz", None),
            P("depth", "horiz", None),
            P("horiz"),
            P(None, "depth"),
            P(None, "depth", None),
        ),
        out_specs=P(None, "depth", "horiz", None),
        check_vma=False,
    )
```

```python
import functools

import jax
import jax.numpy as jnp
from jax import lax
from jax.experimental import pallas as pl
from jax.experimental.pallas import tpu as pltpu
from jax.sharding import PartitionSpec as P

wave_gain = 0.5
SUB = 8
LANE = 128
VMEM = pltpu.VMEM
F32 = jnp.float32
BF16 = jnp.bfloat16


def vmem_spec():
    return pl.BlockSpec(memory_space=VMEM)


def choose(offs, rows):
    value = jnp.broadcast_to(rows[0], offs.shape)
    for o in range(1, len(rows)):
        value = jnp.where(offs == o, jnp.broadcast_to(rows[o], offs.shape), value)
    return value


def split_bf16(x):
    high = x.astype(BF16)
    low = (x - high.astype(F32)).astype(BF16)
    return high, low


def outermost_kernel(
    fields_ref,
    diff_ref,
    offs_hbm,
    coupling_hbm,
    inverse_hbm,
    side_ref,
    far_ref,
    diff_stage_ref,
    offs_ref,
    coupling_ref,
    inverse_ref,
    stage_ref,
    sems,
):
    parts, levels, lines, ny = fields_ref.shape
    even = lax.axis_index("horiz") % 2 == 0
    copies = []
    for e, line in enumerate((0, lines - 1)):
        copy = pltpu.make_async_copy(fields_ref.at[:, :, pl.ds(line, 1), :], stage_ref.at[e], sems.at[e])
        copy.start()
        copies.append(copy)
        copy = pltpu.make_async_copy(diff_ref.at[:, pl.ds(line, 1), :], diff_stage_ref.at[e], sems.at[5 + e])
        copy.start()
        copies.append(copy)
    small = ((offs_hbm, offs_ref), (coupling_hbm, coupling_ref), (inverse_hbm, inverse_ref))
    for n, (source, target) in enumerate(small):
        copy = pltpu.make_async_copy(source, target, sems.at[2 + n])
        copy.start()
        copies.append(copy)
    for copy in copies:
        copy.wait()
    for i in range(parts):
        for c in range(levels // SUB):
            at = slice(c * SUB, (c + 1) * SUB)
            first, last = [gather_rows(lambda k: stage_ref[e, i, k, 0:1, :], c, ny) for e in range(2)]
            side_ref[i, at, :] = jnp.where(even, last, first)
            far_ref[i, at, :] = jnp.where(even, first, last)


def gather_rows(row_at, c, ny):
    sub = lax.broadcasted_iota(jnp.int32, (SUB, ny), 0)
    value = jnp.broadcast_to(row_at(c * SUB), (SUB, ny))
    for t in range(1, SUB):
        value = jnp.where(sub == t, jnp.broadcast_to(row_at(c * SUB + t), value.shape), value)
    return value


def fill_tables(offs_ref, coupling_ref, inverse_ref, offsb_ref, spikes_ref, rows_ref, coefs_ref):
    count, levels, _ = inverse_ref.shape
    lines = offsb_ref.shape[0]
    rank = lax.axis_index("depth")

    square = (lines, lines)
    own = lax.broadcasted_iota(jnp.int32, square, 0) == lax.broadcasted_iota(jnp.int32, square, 1)
    row = jnp.broadcast_to(offs_ref[...].astype(F32), square)
    column = jnp.sum(jnp.where(own, row, jnp.zeros_like(row)), axis=1, keepdims=True)
    offsb_ref[...] = jnp.broadcast_to(column, (lines, LANE)).astype(jnp.int32)

    eye = lax.broadcasted_iota(jnp.int32, (levels, levels), 0) == lax.broadcasted_iota(
        jnp.int32, (levels, levels), 1
    )
    for o in range(count):
        gate = jnp.broadcast_to(coupling_ref[o : o + 1, levels - 1 : levels], (1, LANE))
        face = jnp.broadcast_to(coupling_ref[o : o + 1, 0:1], (1, LANE))
        face = jnp.where(rank > 0, face, jnp.zeros_like(face))
        low = jnp.broadcast_to(inverse_ref[o, :, 0:1], (levels, LANE)) * face
        high = jnp.broadcast_to(inverse_ref[o, :, levels - 2 : levels - 1], (levels, LANE)) * gate
        spikes_ref[0, o] = low
        spikes_ref[1, o] = high
        for k, level in enumerate((0, levels - 2)):
            row = jnp.broadcast_to(inverse_ref[o, level : level + 1, :], (levels, levels))
            column = jnp.sum(jnp.where(eye, row, jnp.zeros_like(row)), axis=1, keepdims=True)
            rows_ref[k, o] = jnp.broadcast_to(column, (levels, LANE))
        b = face - face * low[0:1]
        e = -face * high[0:1]
        l = -gate * low[levels - 2 : levels - 1]
        a = 1.0 + gate - gate * high[levels - 2 : levels - 1]
        for c, row in enumerate((b, e, l, a, gate, face)):
            coefs_ref[c * count + o : c * count + o + 1, :] = row


def force_group(g, fields_ref, diff_ref, offsb_ref, rows_ref, coefs_ref, forcing_ref, sides_ref):
    parts, levels, lines, ny = fields_ref.shape
    groups = lines // SUB
    half = ny // 2
    count = rows_ref.shape[1]
    first = g * SUB
    sub = lax.broadcasted_iota(jnp.int32, (SUB, ny), 0)
    offs = offsb_ref[first : first + SUB, :]
    gate = choose(offs, [coefs_ref[4 * count + o : 4 * count + o + 1, :] for o in range(count)])
    face = choose(offs, [coefs_ref[5 * count + o : 5 * count + o + 1, :] for o in range(count)])

    def one_level(k, sums):
        centre, across, along, both = [], [], [], []
        for i in range(parts):
            c = fields_ref[i, k, first : first + SUB, :]
            north = pltpu.roll(c, ny - 1, 1)
            south = pltpu.roll(c, 1, 1)
            if g > 0:
                row_w = fields_ref[i, k, first - 1 : first, :]
            else:
                row_w = jnp.zeros((1, ny), F32)
            if g < groups - 1:
                row_e = fields_ref[i, k, first + SUB : first + SUB + 1, :]
            else:
                row_e = jnp.zeros((1, ny), F32)
            east = jnp.where(sub == SUB - 1, jnp.broadcast_to(row_e, c.shape), pltpu.roll(c, SUB - 1, 0))
            west = jnp.where(sub == 0, jnp.broadcast_to(row_w, c.shape), pltpu.roll(c, 1, 0))
            centre.append(c)
            both.append((east + west) + (north + south))
            along.append(east - west)
            across.append(north - south)
        d = diff_ref[k, first : first + SUB, :]
        rest = 1.0 - 4.0 * d
        scale = 0.5 * wave_gain
        out = (
            rest * centre[0] + d * both[0] - scale * along[2],
            rest * centre[1] + d * both[1] - scale * across[2],
            rest * centre[2] + d * both[2] - scale * (along[0] + across[1]),
        )
        at = pl.multiple_of(k * SUB, SUB)
        top = choose(offs, [rows_ref[0, o, pl.ds(k, 1), :] for o in range(count)])
        bottom = choose(offs, [rows_ref[1, o, pl.ds(k, 1), :] for o in range(count)])
        new = []
        for i in range(parts):
            forcing_ref[g, i, pl.ds(at, SUB), :] = out[i]
            for h in range(2):
                piece = out[i][:, h * half : (h + 1) * half]
                at_0, at_1 = sums[2 * (i * 2 + h)], sums[2 * (i * 2 + h) + 1]
                new += [at_0 + top * piece, at_1 + bottom * piece]
        return tuple(new)

    def close(sums):
        for i in range(parts):
            for h in range(2):
                cut = slice(h * half, (h + 1) * half)
                last = forcing_ref[g, i, (levels - 1) * SUB :, cut]
                at = i * lines + first
                sides_ref[at : at + SUB, cut] = last + gate * sums[2 * (i * 2 + h) + 1]
                at += parts * lines
                sides_ref[at : at + SUB, cut] = face * sums[2 * (i * 2 + h)]

    return one_level, tuple(jnp.zeros((SUB, half), F32) for _ in range(4 * parts)), close


def run_groups(groups, levels, waits):
    step = levels // len(waits)
    early = groups[:2]
    sums = [start for _, start, _ in early]
    for c, wait in enumerate(waits):
        wait()
        for n, (one_level, _, _) in enumerate(early):
            sums[n] = lax.fori_loop(c * step, (c + 1) * step, one_level, sums[n], unroll=True)
    for total, (_, _, close) in zip(sums, early):
        close(total)
    for one_level, start, close in groups[2:]:
        close(lax.fori_loop(0, levels, one_level, start, unroll=True))


def inner_kernel(
    fields_hbm,
    diff_hbm,
    diff_stage_ref,
    offs_ref,
    coupling_ref,
    inverse_ref,
    offsb_ref,
    spikes_ref,
    rows_ref,
    coefs_ref,
    forcing_ref,
    sides_ref,
    diff_rows_ref,
    fields_ref,
    diff_ref,
    sems,
):
    parts, levels, lines, ny = fields_ref.shape
    chunks = sems.shape[0] // (parts + 1)
    step = levels // chunks
    starts, waits = [], []
    for c in range(chunks):
        at = pl.ds(c * step, step)
        pairs = [(fields_hbm.at[i, at], fields_ref.at[i, at]) for i in range(parts)]
        pairs.append((diff_hbm.at[at], diff_ref.at[at]))
        copies = [
            pltpu.make_async_copy(source, target, sems.at[c * (parts + 1) + n])
            for n, (source, target) in enumerate(pairs)
        ]
        starts.append(lambda copies=copies: [copy.start() for copy in copies])
        waits.append(lambda copies=copies: [copy.wait() for copy in copies])
    for start in starts:
        start()
    fill_tables(offs_ref, coupling_ref, inverse_ref, offsb_ref, spikes_ref, rows_ref, coefs_ref)
    for e in range(2):
        for c in range(levels // SUB):
            diff_rows_ref[e, c * SUB : (c + 1) * SUB, :] = gather_rows(
                lambda k: diff_stage_ref[e, k, 0:1, :], c, ny
            )
    work = [
        force_group(g, fields_ref, diff_ref, offsb_ref, rows_ref, coefs_ref, forcing_ref, sides_ref)
        for g in range(lines // SUB)
    ]
    run_groups(work, levels, waits)


def correct_kernel(
    side_ref, far_ref, sides_ref, diff_rows_ref, offsb_ref, rows_ref, coefs_ref, extra_ref, send_ref, keep_ref
):
    parts, levels, ny = side_ref.shape
    lines = offsb_ref.shape[0]
    half = ny // 2
    count = rows_ref.shape[1]
    core = lax.axis_index("depth") % 2
    even = lax.axis_index("horiz") % 2 == 0
    sub = lax.broadcasted_iota(jnp.int32, (SUB, half), 0)
    scale = 0.5 * wave_gain
    base = 2 * parts * lines
    for at in range(0, base, SUB):
        left, right = sides_ref[at : at + SUB, :half], sides_ref[at : at + SUB, half:]
        keep_ref[at : at + SUB, :] = jnp.where(core == 0, left, right)
        send_ref[at : at + SUB, :] = jnp.where(core == 0, right, left)
    send_ref[base : base + 4 * count, :] = coefs_ref[: 4 * count, :]
    keep_ref[base : base + 4 * count, :] = coefs_ref[: 4 * count, :]

    for e, (line, sign) in enumerate(((0, scale), (lines - 1, -scale))):
        near, other = (far_ref, side_ref) if e == 0 else (side_ref, far_ref)
        halo = [jnp.where(even, near[i], other[i]) for i in range(parts)]
        d = diff_rows_ref[e]
        extra = (d * halo[0] + sign * halo[2], d * halo[1], d * halo[2] + sign * halo[0])
        offs = jnp.broadcast_to(offsb_ref[line : line + 1, :], (levels, half))
        one = offs[:1]
        gate = choose(one, [coefs_ref[4 * count + o : 4 * count + o + 1, :] for o in range(count)])
        face = choose(one, [coefs_ref[5 * count + o : 5 * count + o + 1, :] for o in range(count)])
        top = choose(offs, [rows_ref[0, o] for o in range(count)])
        bottom = choose(offs, [rows_ref[1, o] for o in range(count)])
        group, place = line // SUB * SUB, line % SUB
        for i in range(parts):
            extra_ref[e, i] = extra[i]
            more = []
            for h in range(2):
                piece = extra[i][:, h * half : (h + 1) * half]
                a_side = piece[levels - 1 :, :] + gate * jnp.sum(bottom * piece, axis=0, keepdims=True)
                more.append((a_side, face * jnp.sum(top * piece, axis=0, keepdims=True)))
            for k in range(2):
                left, right = more[0][k], more[1][k]
                at = (k * parts + i) * lines + group
                zero = jnp.zeros((SUB, half), F32)
                for ref, row in (
                    (keep_ref, jnp.where(core == 0, left, right)),
                    (send_ref, jnp.where(core == 0, right, left)),
                ):
                    ref[at : at + SUB, :] += jnp.where(sub == place, jnp.broadcast_to(row, zero.shape), zero)


def block_kernel(
    after_ref, forcing_ref, extra_ref, offsb_ref, inverse_ref, solved_ref, token_ref, wide_ref, big_ref, work_ref
):
    count, levels, _ = inverse_ref.shape
    groups, parts, width, ny = solved_ref.shape
    token_ref[...] = after_ref[:SUB, :]

    spread = (
        lax.broadcasted_iota(jnp.int32, (levels, width), 1) // SUB
        == lax.broadcasted_iota(jnp.int32, (levels, width), 0)
    ).astype(F32)
    for o in range(count):
        wide_ref[o] = lax.dot_general(
            inverse_ref[o],
            spread,
            (((1,), (0,)), ((), ())),
            precision=lax.Precision.HIGHEST,
            preferred_element_type=F32,
        )
    lane = lax.broadcasted_iota(jnp.int32, (SUB, width), 1)
    sub = lax.broadcasted_iota(jnp.int32, (SUB, width), 0)
    diagonal = lane % SUB == sub
    zero = jnp.zeros((SUB, width), F32)
    offs_wide = [
        jnp.concatenate([offsb_ref[g * SUB : (g + 1) * SUB, :]] * (width // LANE), axis=1) for g in range(groups)
    ]

    def one_pair(k, _):
        rows = [[wide_ref[o, pl.ds(2 * k + i, 1), :] for o in range(count)] for i in range(2)]
        for g in range(groups):
            both = jnp.concatenate(
                [jnp.where(diagonal, choose(offs_wide[g], rows[i]), zero) for i in range(2)], axis=0
            )
            high, low = split_bf16(both)
            at = pl.multiple_of(k * 2 * SUB, 2 * SUB)
            big_ref[g, 0, pl.ds(at, 2 * SUB), :] = high
            big_ref[g, 1, pl.ds(at, 2 * SUB), :] = low
        return 0

    lax.fori_loop(0, levels // 2, one_pair, 0)
    here = lax.broadcasted_iota(jnp.int32, (SUB, ny), 0)
    nought = jnp.zeros((SUB, ny), F32)
    for g in range(groups):
        m_high = big_ref[g, 0]
        m_low = big_ref[g, 1]
        for i in range(parts):
            if 0 < g < groups - 1:
                x = forcing_ref[g, i]
            else:
                e, line = (0, 0) if g == 0 else (1, SUB - 1)
                for k in range(levels):
                    at = slice(k * SUB, (k + 1) * SUB)
                    row = jnp.broadcast_to(extra_ref[e, i, k : k + 1, :], (SUB, ny))
                    work_ref[e, i, at, :] = forcing_ref[g, i, at, :] + jnp.where(here == line, row, nought)
                x = work_ref[e, i]
            x_high, x_low = split_bf16(x)
            solved_ref[g, i] = (
                jnp.dot(m_high, x_high, preferred_element_type=F32)
                + jnp.dot(m_low, x_high, preferred_element_type=F32)
                + jnp.dot(m_high, x_low, preferred_element_type=F32)
            )


def unpack(ref, rows, count):
    a_side = ref[:rows, :]
    b_side = ref[rows : 2 * rows, :]
    base = 2 * rows
    b, e, l, a = [ref[base + c * count : base + (c + 1) * count, :] for c in range(4)]
    return a_side, b_side, b, e, l, a


def per_line(offs, table, parts):
    rows = [table[o : o + 1, :] for o in range(table.shape[0])]
    value = choose(offs, rows)
    return jnp.concatenate([value] * parts, axis=0)


def merged(bit, mine_ref, got_ref, offs, parts, count):
    lines = offs.shape[0]
    rows = parts * lines
    lower_is_mine = (lax.axis_index("depth") >> bit) % 2 == 0
    mine = unpack(mine_ref, rows, count)
    got = unpack(got_ref, rows, count)
    a_1, b_1, cb_1, ce_1, cl_1, ca_1 = [jnp.where(lower_is_mine, x, y) for x, y in zip(mine, got)]
    a_2, b_2, cb_2, ce_2, cl_2, ca_2 = [jnp.where(lower_is_mine, y, x) for x, y in zip(mine, got)]
    inverse = 1.0 / (ca_1 + cb_2)
    total = a_1 + b_2
    down = ce_1 * inverse
    up = cl_2 * inverse
    a_new = a_2 - per_line(offs, up, parts) * total
    b_new = b_1 - per_line(offs, down, parts) * total
    cb = cb_1 - down * cl_1
    ce = -down * ce_2
    cl = -up * cl_1
    ca = ca_2 - up * ce_2
    middle = per_line(offs, inverse, parts) * total
    return (a_new, b_new, cb, ce, cl, ca), (middle, cl_1 * inverse, ce_2 * inverse)


def store_saved(saved_ref, saved, count):
    middle, low, high = saved
    rows = middle.shape[0]
    saved_ref[:rows, :] = middle
    saved_ref[rows : rows + count, :] = low
    saved_ref[rows + count : rows + 2 * count, :] = high


def store_element(ref, element, count):
    rows = element[0].shape[0]
    ref[:rows, :] = element[0]
    ref[rows : 2 * rows, :] = element[1]
    for c in range(4):
        ref[2 * rows + c * count : 2 * rows + (c + 1) * count, :] = element[2 + c]


def merge_kernel(bit, parts, count, mine_ref, got_ref, offsb_ref, element_ref, saved_ref):
    element, saved = merged(bit, mine_ref, got_ref, offsb_ref[...], parts, count)
    store_element(element_ref, element, count)
    store_saved(saved_ref, saved, count)


def merge_last_kernel(bit, parts, count, mine_ref, got_ref, offsb_ref, token_ref, element_ref, saved_ref, send_ref):
    offs = offsb_ref[...]
    element, saved = merged(bit, mine_ref, got_ref, offs, parts, count)
    store_element(element_ref, element, count)
    store_saved(saved_ref, saved, count)
    a_side, b_side, cb, ce, cl, ca = element
    rows = a_side.shape[0]
    lower = (lax.axis_index("depth") >> (bit + 1)) == 0
    ratio = ce / ca
    send_ref[:rows, :] = jnp.where(lower, a_side, b_side - per_line(offs, ratio, parts) * a_side)
    send_ref[rows : rows + count, :] = jnp.where(lower, ca, cb - ratio * cl)


def solve_kernel(bits, parts, count, *refs):
    sent_ref, got_ref, element_ref, offsb_ref = refs[:4]
    saved_refs = refs[4 : 4 + bits]
    send_ref, keep_ref = refs[4 + bits :]
    offs = offsb_ref[...]
    rows = parts * offs.shape[0]
    rank = lax.axis_index("depth")
    pivot = sent_ref[rows : rows + count, :] + got_ref[rows : rows + count, :]
    shared = (sent_ref[:rows, :] + got_ref[:rows, :]) * per_line(offs, 1.0 / pivot, parts)
    a_side, _, _, _, cl, ca = unpack(element_ref, rows, count)
    inverse = 1.0 / ca
    top = per_line(offs, inverse, parts) * a_side - per_line(offs, cl * inverse, parts) * shared
    lower = (rank >> bits) == 0
    below = jnp.where(lower, jnp.zeros_like(shared), shared)
    above = jnp.where(lower, shared, top)
    for bit in reversed(range(bits)):
        saved_ref = saved_refs[bit]
        low = saved_ref[rows : rows + count, :]
        high = saved_ref[rows + count : rows + 2 * count, :]
        middle = saved_ref[:rows, :] - per_line(offs, low, parts) * below - per_line(offs, high, parts) * above
        lower = (rank >> bit) % 2 == 0
        if bit > 0:
            below, above = jnp.where(lower, below, middle), jnp.where(lower, middle, above)
        else:
            keep_ref[:rows, :] = jnp.where(lower, below, middle)
            keep_ref[rows:, :] = jnp.where(lower, middle, above)
            send_ref[:rows, :] = jnp.where(lower, middle, below)
            send_ref[rows:, :] = jnp.where(lower, above, middle)


def finish_kernel(step, own, solved_ref, ends_ref, offsb_ref, spikes_ref, *refs):
    out_ref, stage_ref, sems = refs[-3:]
    parts, levels, lines, ny = out_ref.shape
    groups = lines // SUB
    half = ny // 2
    count = spikes_ref.shape[1]
    rows = parts * lines
    core = lax.axis_index("depth") % 2
    cut = pl.ds(pl.multiple_of((core if own else 1 - core) * half, half), half)

    copies = []
    for c in range(levels // step):
        for g in range(groups):
            lane = slice(g * SUB, (g + 1) * SUB)
            offs = offsb_ref[lane, :]
            side = [
                [ends_ref[k * rows + i * lines + g * SUB : k * rows + i * lines + (g + 1) * SUB, :] for i in range(parts)]
                for k in range(2)
            ]
            for k in range(c * step, (c + 1) * step):
                if k == levels - 1:
                    for i in range(parts):
                        stage_ref[i, k, lane, :] = side[1][i]
                    continue
                low = choose(offs, [spikes_ref[0, o, k : k + 1, :] for o in range(count)])
                high = choose(offs, [spikes_ref[1, o, k : k + 1, :] for o in range(count)])
                for i in range(parts):
                    value = solved_ref[g, i, k * SUB : (k + 1) * SUB, cut]
                    stage_ref[i, k, lane, :] = value + low * side[0][i] + high * side[1][i]
        for i in range(parts):
            at = pl.ds(c * step, step)
            copy = pltpu.make_async_copy(stage_ref.at[i, at], out_ref.at[i, at, :, cut], sems.at[c * parts + i])
            copy.start()
            copies.append(copy)
    for copy in copies:
        copy.wait()


def call(kernel, outs, args, scratch=(), specs=None, **options):
    put = [pltpu.with_memory_space_constraint(x, VMEM) for x in args] if specs is None else args
    return pl.pallas_call(
        kernel,
        out_shape=[VMEM(s, d) for s, d in outs],
        in_specs=specs or [vmem_spec()] * len(args),
        out_specs=[vmem_spec()] * len(outs),
        scratch_shapes=list(scratch),
        compiler_params=pltpu.CompilerParams(vmem_limit_bytes=16 * 2**20),
    )(*put)


def finish(own, out_shape, args, before=None):
    step = SUB
    parts, levels, lines, ny = out_shape
    put = [pltpu.with_memory_space_constraint(x, VMEM) for x in args]
    specs = [vmem_spec()] * len(args)
    aliases = {}
    if before is not None:
        put.append(pltpu.with_memory_space_constraint(before, pltpu.HBM))
        specs.append(pl.BlockSpec(memory_space=pltpu.HBM))
        aliases = {len(args): 0}
    return pl.pallas_call(
        functools.partial(finish_kernel, step, own),
        out_shape=pltpu.HBM(out_shape, F32),
        in_specs=specs,
        out_specs=pl.BlockSpec(memory_space=pltpu.HBM),
        scratch_shapes=[
            pltpu.VMEM((parts, levels, lines, ny // 2), F32),
            pltpu.SemaphoreType.DMA((parts * (levels // step),)),
        ],
        input_output_aliases=aliases,
        compiler_params=pltpu.CompilerParams(vmem_limit_bytes=16 * 2**20),
    )(*put)


def body(fields, diffusivity, offsets, coupling, inverse):
    parts, levels, lines, ny = fields.shape
    count = inverse.shape[0]
    half = ny // 2
    groups = lines // SUB
    width = levels * SUB
    around = lax.axis_size("horiz")
    ranks = lax.axis_size("depth")
    bits = ranks.bit_length() - 1
    assert ranks == 1 << bits and bits >= 2 and around % 2 == 0 and half == LANE and groups >= 2

    def swap(x, bit):
        return lax.ppermute(x, "depth", [(i, i ^ (1 << bit)) for i in range(ranks)])

    in_hbm = pl.BlockSpec(memory_space=pltpu.HBM)
    edge = ((parts, levels, ny), F32)
    offsets = offsets.reshape(1, lines)
    to_side, to_far, diff_stage, offsets, coupling, inverse = call(
        outermost_kernel,
        [edge, edge, ((2, levels, 1, ny), F32), (offsets.shape, jnp.int32), (coupling.shape, F32), (inverse.shape, F32)],
        [pltpu.with_memory_space_constraint(x, pltpu.HBM) for x in (fields, diffusivity, offsets, coupling, inverse)],
        scratch=[
            pltpu.VMEM((2, parts, levels, 1, ny), F32),
            pltpu.SemaphoreType.DMA((7,)),
        ],
        specs=[in_hbm] * 5,
    )
    far = lax.ppermute(to_far, "horiz", [(i, (i + 2 * (i % 2) - 1) % around) for i in range(around)])
    side = lax.ppermute(to_side, "horiz", [(i, (i + 1 - 2 * (i % 2)) % around) for i in range(around)])

    rows = parts * lines
    table = ((2, count, levels, LANE), F32)
    offsb, spikes, k_rows, coefs, forcing, sides, diff_rows = call(
        inner_kernel,
        [
            ((lines, LANE), jnp.int32),
            table,
            table,
            ((6 * count, LANE), F32),
            ((groups, parts, width, ny), F32),
            ((2 * rows, ny), F32),
            ((2, levels, ny), F32),
        ],
        [pltpu.with_memory_space_constraint(x, pltpu.HBM) for x in (fields, diffusivity)]
        + [diff_stage, offsets, coupling, inverse],
        scratch=[
            pltpu.VMEM(fields.shape, F32),
            pltpu.VMEM(diffusivity.shape, F32),
            pltpu.SemaphoreType.DMA(((parts + 1) * (levels // SUB),)),
        ],
        specs=[in_hbm] * 2 + [vmem_spec()] * 4,
    )
    element_shape = ((2 * rows + 4 * count, half), F32)
    saved_shape = ((rows + 2 * count, half), F32)
    extra, send, mine = call(
        correct_kernel,
        [((2, parts, levels, ny), F32), element_shape, element_shape],
        (side, far, sides, diff_rows, offsb, k_rows, coefs),
    )
    got = swap(send, 0)
    saved = []
    for bit in range(bits - 1):
        if bit < bits - 2:
            mine, kept = call(
                functools.partial(merge_kernel, bit, parts, count),
                [element_shape, saved_shape],
                (mine, got, offsb),
            )
            got = swap(mine, bit + 1)
        if bit == 0:
            solved, token = call(
                block_kernel,
                [((groups, parts, width, ny), F32), ((SUB, LANE), F32)],
                (mine, forcing, extra, offsb, inverse),
                scratch=[
                    pltpu.VMEM((count, levels, width), F32),
                    pltpu.VMEM((groups, 2, width, width), BF16),
                    pltpu.VMEM((2, parts, width, ny), F32),
                ],
            )
        if bit == bits - 2:
            mine, kept, send = call(
                functools.partial(merge_last_kernel, bit, parts, count),
                [element_shape, saved_shape, ((rows + count, half), F32)],
                (mine, got, offsb, token),
            )
            got = swap(send, bit + 1)
        saved.append(kept)
    pair = ((2 * rows, half), F32)
    theirs, own = call(
        functools.partial(solve_kernel, bits - 1, parts, count),
        [pair, pair],
        (send, got, mine, offsb, *saved),
    )
    other = swap(theirs, 0)
    half_out = finish(True, (parts, levels, lines, ny), (solved, own, offsb, spikes))
    return finish(False, (parts, levels, lines, ny), (solved, other, offsb, spikes), half_out)


def solution(mesh):
    return jax.shard_map(
        body,
        mesh=mesh,
        in_specs=(
            P(None, "depth", "horiz", None),
            P("depth", "horiz", None),
            P("horiz"),
            P(None, "depth"),
            P(None, "depth", None),
        ),
        out_specs=P(None, "depth", "horiz", None),
        check_vma=False,
    )
```

```python
import functools

import jax
import jax.numpy as jnp
from jax import lax
from jax.experimental import pallas as pl
from jax.experimental.pallas import tpu as pltpu
from jax.sharding import PartitionSpec as P

wave_gain = 0.5
SUB = 8
LANE = 128
VMEM = pltpu.VMEM
F32 = jnp.float32
BF16 = jnp.bfloat16


def vmem_spec():
    return pl.BlockSpec(memory_space=VMEM)


def choose(offs, rows):
    value = jnp.broadcast_to(rows[0], offs.shape)
    for o in range(1, len(rows)):
        value = jnp.where(offs == o, jnp.broadcast_to(rows[o], offs.shape), value)
    return value


def split_bf16(x):
    high = x.astype(BF16)
    low = (x - high.astype(F32)).astype(BF16)
    return high, low


def outermost_kernel(
    fields_ref,
    diff_ref,
    offs_hbm,
    coupling_hbm,
    inverse_hbm,
    side_ref,
    far_ref,
    diff_stage_ref,
    offs_ref,
    coupling_ref,
    inverse_ref,
    stage_ref,
    sems,
):
    parts, levels, lines, ny = fields_ref.shape
    even = lax.axis_index("horiz") % 2 == 0
    copies = []
    for e, line in enumerate((0, lines - 1)):
        copy = pltpu.make_async_copy(fields_ref.at[:, :, pl.ds(line, 1), :], stage_ref.at[e], sems.at[e])
        copy.start()
        copies.append(copy)
    for e, line in enumerate((0, lines - 1)):
        copy = pltpu.make_async_copy(diff_ref.at[:, pl.ds(line, 1), :], diff_stage_ref.at[e], sems.at[5 + e])
        copy.start()
        copies.append(copy)
    small = ((offs_hbm, offs_ref), (coupling_hbm, coupling_ref), (inverse_hbm, inverse_ref))
    for n, (source, target) in enumerate(small):
        copy = pltpu.make_async_copy(source, target, sems.at[2 + n])
        copy.start()
        copies.append(copy)
    for copy in copies[:2]:
        copy.wait()
    for i in range(parts):
        for c in range(levels // SUB):
            at = slice(c * SUB, (c + 1) * SUB)
            first, last = [gather_rows(lambda k: stage_ref[e, i, k, 0:1, :], c, ny) for e in range(2)]
            side_ref[i, at, :] = jnp.where(even, last, first)
            far_ref[i, at, :] = jnp.where(even, first, last)
    for copy in copies[2:]:
        copy.wait()


def gather_rows(row_at, c, ny):
    sub = lax.broadcasted_iota(jnp.int32, (SUB, ny), 0)
    value = jnp.broadcast_to(row_at(c * SUB), (SUB, ny))
    for t in range(1, SUB):
        value = jnp.where(sub == t, jnp.broadcast_to(row_at(c * SUB + t), value.shape), value)
    return value


def fill_tables(offs_ref, coupling_ref, inverse_ref, offsb_ref, spikes_ref, rows_ref, coefs_ref):
    count, levels, _ = inverse_ref.shape
    lines = offsb_ref.shape[0]
    rank = lax.axis_index("depth")

    square = (lines, lines)
    own = lax.broadcasted_iota(jnp.int32, square, 0) == lax.broadcasted_iota(jnp.int32, square, 1)
    row = jnp.broadcast_to(offs_ref[...].astype(F32), square)
    column = jnp.sum(jnp.where(own, row, jnp.zeros_like(row)), axis=1, keepdims=True)
    offsb_ref[...] = jnp.broadcast_to(column, (lines, LANE)).astype(jnp.int32)

    eye = lax.broadcasted_iota(jnp.int32, (levels, levels), 0) == lax.broadcasted_iota(
        jnp.int32, (levels, levels), 1
    )
    for o in range(count):
        gate = jnp.broadcast_to(coupling_ref[o : o + 1, levels - 1 : levels], (1, LANE))
        face = jnp.broadcast_to(coupling_ref[o : o + 1, 0:1], (1, LANE))
        face = jnp.where(rank > 0, face, jnp.zeros_like(face))
        low = jnp.broadcast_to(inverse_ref[o, :, 0:1], (levels, LANE)) * face
        high = jnp.broadcast_to(inverse_ref[o, :, levels - 2 : levels - 1], (levels, LANE)) * gate
        spikes_ref[0, o] = low
        spikes_ref[1, o] = high
        for k, level in enumerate((0, levels - 2)):
            row = jnp.broadcast_to(inverse_ref[o, level : level + 1, :], (levels, levels))
            column = jnp.sum(jnp.where(eye, row, jnp.zeros_like(row)), axis=1, keepdims=True)
            rows_ref[k, o] = jnp.broadcast_to(column, (levels, LANE))
        b = face - face * low[0:1]
        e = -face * high[0:1]
        l = -gate * low[levels - 2 : levels - 1]
        a = 1.0 + gate - gate * high[levels - 2 : levels - 1]
        for c, row in enumerate((b, e, l, a, gate, face)):
            coefs_ref[c * count + o : c * count + o + 1, :] = row


def force_group(g, fields_ref, diff_ref, offsb_ref, rows_ref, coefs_ref, forcing_ref, sides_ref):
    parts, levels, lines, ny = fields_ref.shape
    groups = lines // SUB
    half = ny // 2
    count = rows_ref.shape[1]
    first = g * SUB
    sub = lax.broadcasted_iota(jnp.int32, (SUB, ny), 0)
    offs = offsb_ref[first : first + SUB, :]
    gate = choose(offs, [coefs_ref[4 * count + o : 4 * count + o + 1, :] for o in range(count)])
    face = choose(offs, [coefs_ref[5 * count + o : 5 * count + o + 1, :] for o in range(count)])

    def one_level(k, sums):
        centre, across, along, both = [], [], [], []
        for i in range(parts):
            c = fields_ref[i, k, first : first + SUB, :]
            north = pltpu.roll(c, ny - 1, 1)
            south = pltpu.roll(c, 1, 1)
            if g > 0:
                row_w = fields_ref[i, k, first - 1 : first, :]
            else:
                row_w = jnp.zeros((1, ny), F32)
            if g < groups - 1:
                row_e = fields_ref[i, k, first + SUB : first + SUB + 1, :]
            else:
                row_e = jnp.zeros((1, ny), F32)
            east = jnp.where(sub == SUB - 1, jnp.broadcast_to(row_e, c.shape), pltpu.roll(c, SUB - 1, 0))
            west = jnp.where(sub == 0, jnp.broadcast_to(row_w, c.shape), pltpu.roll(c, 1, 0))
            centre.append(c)
            both.append((east + west) + (north + south))
            along.append(east - west)
            across.append(north - south)
        d = diff_ref[k, first : first + SUB, :]
        rest = 1.0 - 4.0 * d
        scale = 0.5 * wave_gain
        out = (
            rest * centre[0] + d * both[0] - scale * along[2],
            rest * centre[1] + d * both[1] - scale * across[2],
            rest * centre[2] + d * both[2] - scale * (along[0] + across[1]),
        )
        at = pl.multiple_of(k * SUB, SUB)
        top = choose(offs, [rows_ref[0, o, pl.ds(k, 1), :] for o in range(count)])
        bottom = choose(offs, [rows_ref[1, o, pl.ds(k, 1), :] for o in range(count)])
        new = []
        for i in range(parts):
            forcing_ref[g, i, pl.ds(at, SUB), :] = out[i]
            for h in range(2):
                piece = out[i][:, h * half : (h + 1) * half]
                at_0, at_1 = sums[2 * (i * 2 + h)], sums[2 * (i * 2 + h) + 1]
                new += [at_0 + top * piece, at_1 + bottom * piece]
        return tuple(new)

    def close(sums):
        for i in range(parts):
            for h in range(2):
                cut = slice(h * half, (h + 1) * half)
                last = forcing_ref[g, i, (levels - 1) * SUB :, cut]
                at = i * lines + first
                sides_ref[at : at + SUB, cut] = last + gate * sums[2 * (i * 2 + h) + 1]
                at += parts * lines
                sides_ref[at : at + SUB, cut] = face * sums[2 * (i * 2 + h)]

    return one_level, tuple(jnp.zeros((SUB, half), F32) for _ in range(4 * parts)), close


def run_groups(groups, levels, waits):
    step = levels // len(waits)
    early = groups[:2]
    sums = [start for _, start, _ in early]
    for c, wait in enumerate(waits):
        wait()
        for n, (one_level, _, _) in enumerate(early):
            sums[n] = lax.fori_loop(c * step, (c + 1) * step, one_level, sums[n], unroll=True)
    for total, (_, _, close) in zip(sums, early):
        close(total)
    for one_level, start, close in groups[2:]:
        close(lax.fori_loop(0, levels, one_level, start, unroll=True))


def inner_kernel(
    fields_hbm,
    diff_hbm,
    diff_stage_ref,
    offs_ref,
    coupling_ref,
    inverse_ref,
    offsb_ref,
    spikes_ref,
    rows_ref,
    coefs_ref,
    forcing_ref,
    sides_ref,
    diff_rows_ref,
    fields_ref,
    diff_ref,
    sems,
):
    parts, levels, lines, ny = fields_ref.shape
    chunks = sems.shape[0] // (parts + 1)
    step = levels // chunks
    starts, waits = [], []
    for c in range(chunks):
        at = pl.ds(c * step, step)
        pairs = [(fields_hbm.at[i, at], fields_ref.at[i, at]) for i in range(parts)]
        pairs.append((diff_hbm.at[at], diff_ref.at[at]))
        copies = [
            pltpu.make_async_copy(source, target, sems.at[c * (parts + 1) + n])
            for n, (source, target) in enumerate(pairs)
        ]
        starts.append(lambda copies=copies: [copy.start() for copy in copies])
        waits.append(lambda copies=copies: [copy.wait() for copy in copies])
    for start in starts:
        start()
    fill_tables(offs_ref, coupling_ref, inverse_ref, offsb_ref, spikes_ref, rows_ref, coefs_ref)
    for e in range(2):
        for c in range(levels // SUB):
            diff_rows_ref[e, c * SUB : (c + 1) * SUB, :] = gather_rows(
                lambda k: diff_stage_ref[e, k, 0:1, :], c, ny
            )
    work = [
        force_group(g, fields_ref, diff_ref, offsb_ref, rows_ref, coefs_ref, forcing_ref, sides_ref)
        for g in range(lines // SUB)
    ]
    run_groups(work, levels, waits)


def correct_kernel(
    side_ref, far_ref, sides_ref, diff_rows_ref, offsb_ref, rows_ref, coefs_ref, extra_ref, send_ref, keep_ref
):
    parts, levels, ny = side_ref.shape
    lines = offsb_ref.shape[0]
    half = ny // 2
    count = rows_ref.shape[1]
    core = lax.axis_index("depth") % 2
    even = lax.axis_index("horiz") % 2 == 0
    sub = lax.broadcasted_iota(jnp.int32, (SUB, half), 0)
    scale = 0.5 * wave_gain
    base = 2 * parts * lines
    for at in range(0, base, SUB):
        left, right = sides_ref[at : at + SUB, :half], sides_ref[at : at + SUB, half:]
        keep_ref[at : at + SUB, :] = jnp.where(core == 0, left, right)
        send_ref[at : at + SUB, :] = jnp.where(core == 0, right, left)
    send_ref[base : base + 4 * count, :] = coefs_ref[: 4 * count, :]
    keep_ref[base : base + 4 * count, :] = coefs_ref[: 4 * count, :]

    for e, (line, sign) in enumerate(((0, scale), (lines - 1, -scale))):
        near, other = (far_ref, side_ref) if e == 0 else (side_ref, far_ref)
        halo = [jnp.where(even, near[i], other[i]) for i in range(parts)]
        d = diff_rows_ref[e]
        extra = (d * halo[0] + sign * halo[2], d * halo[1], d * halo[2] + sign * halo[0])
        offs = jnp.broadcast_to(offsb_ref[line : line + 1, :], (levels, half))
        one = offs[:1]
        gate = choose(one, [coefs_ref[4 * count + o : 4 * count + o + 1, :] for o in range(count)])
        face = choose(one, [coefs_ref[5 * count + o : 5 * count + o + 1, :] for o in range(count)])
        top = choose(offs, [rows_ref[0, o] for o in range(count)])
        bottom = choose(offs, [rows_ref[1, o] for o in range(count)])
        group, place = line // SUB * SUB, line % SUB
        for i in range(parts):
            extra_ref[e, i] = extra[i]
            more = []
            for h in range(2):
                piece = extra[i][:, h * half : (h + 1) * half]
                a_side = piece[levels - 1 :, :] + gate * jnp.sum(bottom * piece, axis=0, keepdims=True)
                more.append((a_side, face * jnp.sum(top * piece, axis=0, keepdims=True)))
            for k in range(2):
                left, right = more[0][k], more[1][k]
                at = (k * parts + i) * lines + group
                zero = jnp.zeros((SUB, half), F32)
                for ref, row in (
                    (keep_ref, jnp.where(core == 0, left, right)),
                    (send_ref, jnp.where(core == 0, right, left)),
                ):
                    ref[at : at + SUB, :] += jnp.where(sub == place, jnp.broadcast_to(row, zero.shape), zero)


def block_kernel(
    after_ref, forcing_ref, extra_ref, offsb_ref, inverse_ref, solved_ref, token_ref, wide_ref, big_ref, work_ref
):
    count, levels, _ = inverse_ref.shape
    groups, parts, width, ny = solved_ref.shape
    token_ref[...] = after_ref[:SUB, :]

    spread = (
        lax.broadcasted_iota(jnp.int32, (levels, width), 1) // SUB
        == lax.broadcasted_iota(jnp.int32, (levels, width), 0)
    ).astype(F32)
    for o in range(count):
        wide_ref[o] = lax.dot_general(
            inverse_ref[o],
            spread,
            (((1,), (0,)), ((), ())),
            precision=lax.Precision.HIGHEST,
            preferred_element_type=F32,
        )
    lane = lax.broadcasted_iota(jnp.int32, (SUB, width), 1)
    sub = lax.broadcasted_iota(jnp.int32, (SUB, width), 0)
    diagonal = lane % SUB == sub
    zero = jnp.zeros((SUB, width), F32)
    offs_wide = [
        jnp.concatenate([offsb_ref[g * SUB : (g + 1) * SUB, :]] * (width // LANE), axis=1) for g in range(groups)
    ]

    def one_pair(k, _):
        rows = [[wide_ref[o, pl.ds(2 * k + i, 1), :] for o in range(count)] for i in range(2)]
        for g in range(groups):
            both = jnp.concatenate(
                [jnp.where(diagonal, choose(offs_wide[g], rows[i]), zero) for i in range(2)], axis=0
            )
            high, low = split_bf16(both)
            at = pl.multiple_of(k * 2 * SUB, 2 * SUB)
            big_ref[g, 0, pl.ds(at, 2 * SUB), :] = high
            big_ref[g, 1, pl.ds(at, 2 * SUB), :] = low
        return 0

    lax.fori_loop(0, levels // 2, one_pair, 0)
    here = lax.broadcasted_iota(jnp.int32, (SUB, ny), 0)
    nought = jnp.zeros((SUB, ny), F32)
    for g in range(groups):
        m_high = big_ref[g, 0]
        m_low = big_ref[g, 1]
        for i in range(parts):
            if 0 < g < groups - 1:
                x = forcing_ref[g, i]
            else:
                e, line = (0, 0) if g == 0 else (1, SUB - 1)
                for k in range(levels):
                    at = slice(k * SUB, (k + 1) * SUB)
                    row = jnp.broadcast_to(extra_ref[e, i, k : k + 1, :], (SUB, ny))
                    work_ref[e, i, at, :] = forcing_ref[g, i, at, :] + jnp.where(here == line, row, nought)
                x = work_ref[e, i]
            x_high, x_low = split_bf16(x)
            solved_ref[g, i] = (
                jnp.dot(m_high, x_high, preferred_element_type=F32)
                + jnp.dot(m_low, x_high, preferred_element_type=F32)
                + jnp.dot(m_high, x_low, preferred_element_type=F32)
            )


def unpack(ref, rows, count):
    a_side = ref[:rows, :]
    b_side = ref[rows : 2 * rows, :]
    base = 2 * rows
    b, e, l, a = [ref[base + c * count : base + (c + 1) * count, :] for c in range(4)]
    return a_side, b_side, b, e, l, a


def per_line(offs, table, parts):
    rows = [table[o : o + 1, :] for o in range(table.shape[0])]
    value = choose(offs, rows)
    return jnp.concatenate([value] * parts, axis=0)


def merged(bit, mine_ref, got_ref, offs, parts, count):
    lines = offs.shape[0]
    rows = parts * lines
    lower_is_mine = (lax.axis_index("depth") >> bit) % 2 == 0
    mine = unpack(mine_ref, rows, count)
    got = unpack(got_ref, rows, count)
    a_1, b_1, cb_1, ce_1, cl_1, ca_1 = [jnp.where(lower_is_mine, x, y) for x, y in zip(mine, got)]
    a_2, b_2, cb_2, ce_2, cl_2, ca_2 = [jnp.where(lower_is_mine, y, x) for x, y in zip(mine, got)]
    inverse = 1.0 / (ca_1 + cb_2)
    total = a_1 + b_2
    down = ce_1 * inverse
    up = cl_2 * inverse
    a_new = a_2 - per_line(offs, up, parts) * total
    b_new = b_1 - per_line(offs, down, parts) * total
    cb = cb_1 - down * cl_1
    ce = -down * ce_2
    cl = -up * cl_1
    ca = ca_2 - up * ce_2
    middle = per_line(offs, inverse, parts) * total
    return (a_new, b_new, cb, ce, cl, ca), (middle, cl_1 * inverse, ce_2 * inverse)


def store_saved(saved_ref, saved, count):
    middle, low, high = saved
    rows = middle.shape[0]
    saved_ref[:rows, :] = middle
    saved_ref[rows : rows + count, :] = low
    saved_ref[rows + count : rows + 2 * count, :] = high


def store_element(ref, element, count):
    rows = element[0].shape[0]
    ref[:rows, :] = element[0]
    ref[rows : 2 * rows, :] = element[1]
    for c in range(4):
        ref[2 * rows + c * count : 2 * rows + (c + 1) * count, :] = element[2 + c]


def merge_kernel(bit, parts, count, mine_ref, got_ref, offsb_ref, element_ref, saved_ref):
    element, saved = merged(bit, mine_ref, got_ref, offsb_ref[...], parts, count)
    store_element(element_ref, element, count)
    store_saved(saved_ref, saved, count)


def merge_last_kernel(bit, parts, count, mine_ref, got_ref, offsb_ref, token_ref, element_ref, saved_ref, send_ref):
    offs = offsb_ref[...]
    element, saved = merged(bit, mine_ref, got_ref, offs, parts, count)
    store_element(element_ref, element, count)
    store_saved(saved_ref, saved, count)
    a_side, b_side, cb, ce, cl, ca = element
    rows = a_side.shape[0]
    lower = (lax.axis_index("depth") >> (bit + 1)) == 0
    ratio = ce / ca
    send_ref[:rows, :] = jnp.where(lower, a_side, b_side - per_line(offs, ratio, parts) * a_side)
    send_ref[rows : rows + count, :] = jnp.where(lower, ca, cb - ratio * cl)


def solve_kernel(bits, parts, count, *refs):
    sent_ref, got_ref, element_ref, offsb_ref = refs[:4]
    saved_refs = refs[4 : 4 + bits]
    send_ref, keep_ref = refs[4 + bits :]
    offs = offsb_ref[...]
    rows = parts * offs.shape[0]
    rank = lax.axis_index("depth")
    pivot = sent_ref[rows : rows + count, :] + got_ref[rows : rows + count, :]
    shared = (sent_ref[:rows, :] + got_ref[:rows, :]) * per_line(offs, 1.0 / pivot, parts)
    a_side, _, _, _, cl, ca = unpack(element_ref, rows, count)
    inverse = 1.0 / ca
    top = per_line(offs, inverse, parts) * a_side - per_line(offs, cl * inverse, parts) * shared
    lower = (rank >> bits) == 0
    below = jnp.where(lower, jnp.zeros_like(shared), shared)
    above = jnp.where(lower, shared, top)
    for bit in reversed(range(bits)):
        saved_ref = saved_refs[bit]
        low = saved_ref[rows : rows + count, :]
        high = saved_ref[rows + count : rows + 2 * count, :]
        middle = saved_ref[:rows, :] - per_line(offs, low, parts) * below - per_line(offs, high, parts) * above
        lower = (rank >> bit) % 2 == 0
        if bit > 0:
            below, above = jnp.where(lower, below, middle), jnp.where(lower, middle, above)
        else:
            keep_ref[:rows, :] = jnp.where(lower, below, middle)
            keep_ref[rows:, :] = jnp.where(lower, middle, above)
            send_ref[:rows, :] = jnp.where(lower, middle, below)
            send_ref[rows:, :] = jnp.where(lower, above, middle)


def finish_kernel(step, own, solved_ref, ends_ref, offsb_ref, spikes_ref, *refs):
    out_ref, stage_ref, sems = refs[-3:]
    parts, levels, lines, ny = out_ref.shape
    groups = lines // SUB
    half = ny // 2
    count = spikes_ref.shape[1]
    rows = parts * lines
    core = lax.axis_index("depth") % 2
    cut = pl.ds(pl.multiple_of((core if own else 1 - core) * half, half), half)

    copies = []
    for c in range(levels // step):
        for g in range(groups):
            lane = slice(g * SUB, (g + 1) * SUB)
            offs = offsb_ref[lane, :]
            side = [
                [ends_ref[k * rows + i * lines + g * SUB : k * rows + i * lines + (g + 1) * SUB, :] for i in range(parts)]
                for k in range(2)
            ]
            for k in range(c * step, (c + 1) * step):
                if k == levels - 1:
                    for i in range(parts):
                        stage_ref[i, k, lane, :] = side[1][i]
                    continue
                low = choose(offs, [spikes_ref[0, o, k : k + 1, :] for o in range(count)])
                high = choose(offs, [spikes_ref[1, o, k : k + 1, :] for o in range(count)])
                for i in range(parts):
                    value = solved_ref[g, i, k * SUB : (k + 1) * SUB, cut]
                    stage_ref[i, k, lane, :] = value + low * side[0][i] + high * side[1][i]
        for i in range(parts):
            at = pl.ds(c * step, step)
            copy = pltpu.make_async_copy(stage_ref.at[i, at], out_ref.at[i, at, :, cut], sems.at[c * parts + i])
            copy.start()
            copies.append(copy)
    for copy in copies:
        copy.wait()


def call(kernel, outs, args, scratch=(), specs=None, **options):
    put = [pltpu.with_memory_space_constraint(x, VMEM) for x in args] if specs is None else args
    return pl.pallas_call(
        kernel,
        out_shape=[VMEM(s, d) for s, d in outs],
        in_specs=specs or [vmem_spec()] * len(args),
        out_specs=[vmem_spec()] * len(outs),
        scratch_shapes=list(scratch),
        compiler_params=pltpu.CompilerParams(vmem_limit_bytes=16 * 2**20),
    )(*put)


def finish(own, out_shape, args, before=None):
    step = SUB
    parts, levels, lines, ny = out_shape
    put = [pltpu.with_memory_space_constraint(x, VMEM) for x in args]
    specs = [vmem_spec()] * len(args)
    aliases = {}
    if before is not None:
        put.append(pltpu.with_memory_space_constraint(before, pltpu.HBM))
        specs.append(pl.BlockSpec(memory_space=pltpu.HBM))
        aliases = {len(args): 0}
    return pl.pallas_call(
        functools.partial(finish_kernel, step, own),
        out_shape=pltpu.HBM(out_shape, F32),
        in_specs=specs,
        out_specs=pl.BlockSpec(memory_space=pltpu.HBM),
        scratch_shapes=[
            pltpu.VMEM((parts, levels, lines, ny // 2), F32),
            pltpu.SemaphoreType.DMA((parts * (levels // step),)),
        ],
        input_output_aliases=aliases,
        compiler_params=pltpu.CompilerParams(vmem_limit_bytes=16 * 2**20),
    )(*put)


def body(fields, diffusivity, offsets, coupling, inverse):
    parts, levels, lines, ny = fields.shape
    count = inverse.shape[0]
    half = ny // 2
    groups = lines // SUB
    width = levels * SUB
    around = lax.axis_size("horiz")
    ranks = lax.axis_size("depth")
    bits = ranks.bit_length() - 1
    assert ranks == 1 << bits and bits >= 2 and around % 2 == 0 and half == LANE and groups >= 2

    def swap(x, bit):
        return lax.ppermute(x, "depth", [(i, i ^ (1 << bit)) for i in range(ranks)])

    in_hbm = pl.BlockSpec(memory_space=pltpu.HBM)
    edge = ((parts, levels, ny), F32)
    offsets = offsets.reshape(1, lines)
    to_side, to_far, diff_stage, offsets, coupling, inverse = call(
        outermost_kernel,
        [edge, edge, ((2, levels, 1, ny), F32), (offsets.shape, jnp.int32), (coupling.shape, F32), (inverse.shape, F32)],
        [pltpu.with_memory_space_constraint(x, pltpu.HBM) for x in (fields, diffusivity, offsets, coupling, inverse)],
        scratch=[
            pltpu.VMEM((2, parts, levels, 1, ny), F32),
            pltpu.SemaphoreType.DMA((7,)),
        ],
        specs=[in_hbm] * 5,
    )
    far = lax.ppermute(to_far, "horiz", [(i, (i + 2 * (i % 2) - 1) % around) for i in range(around)])
    side = lax.ppermute(to_side, "horiz", [(i, (i + 1 - 2 * (i % 2)) % around) for i in range(around)])

    rows = parts * lines
    table = ((2, count, levels, LANE), F32)
    offsb, spikes, k_rows, coefs, forcing, sides, diff_rows = call(
        inner_kernel,
        [
            ((lines, LANE), jnp.int32),
            table,
            table,
            ((6 * count, LANE), F32),
            ((groups, parts, width, ny), F32),
            ((2 * rows, ny), F32),
            ((2, levels, ny), F32),
        ],
        [pltpu.with_memory_space_constraint(x, pltpu.HBM) for x in (fields, diffusivity)]
        + [diff_stage, offsets, coupling, inverse],
        scratch=[
            pltpu.VMEM(fields.shape, F32),
            pltpu.VMEM(diffusivity.shape, F32),
            pltpu.SemaphoreType.DMA(((parts + 1) * (levels // SUB),)),
        ],
        specs=[in_hbm] * 2 + [vmem_spec()] * 4,
    )
    element_shape = ((2 * rows + 4 * count, half), F32)
    saved_shape = ((rows + 2 * count, half), F32)
    extra, send, mine = call(
        correct_kernel,
        [((2, parts, levels, ny), F32), element_shape, element_shape],
        (side, far, sides, diff_rows, offsb, k_rows, coefs),
    )
    got = swap(send, 0)
    saved = []
    for bit in range(bits - 1):
        if bit < bits - 2:
            mine, kept = call(
                functools.partial(merge_kernel, bit, parts, count),
                [element_shape, saved_shape],
                (mine, got, offsb),
            )
            got = swap(mine, bit + 1)
        if bit == 0:
            solved, token = call(
                block_kernel,
                [((groups, parts, width, ny), F32), ((SUB, LANE), F32)],
                (mine, forcing, extra, offsb, inverse),
                scratch=[
                    pltpu.VMEM((count, levels, width), F32),
                    pltpu.VMEM((groups, 2, width, width), BF16),
                    pltpu.VMEM((2, parts, width, ny), F32),
                ],
            )
        if bit == bits - 2:
            mine, kept, send = call(
                functools.partial(merge_last_kernel, bit, parts, count),
                [element_shape, saved_shape, ((rows + count, half), F32)],
                (mine, got, offsb, token),
            )
            got = swap(send, bit + 1)
        saved.append(kept)
    pair = ((2 * rows, half), F32)
    theirs, own = call(
        functools.partial(solve_kernel, bits - 1, parts, count),
        [pair, pair],
        (send, got, mine, offsb, *saved),
    )
    other = swap(theirs, 0)
    half_out = finish(True, (parts, levels, lines, ny), (solved, own, offsb, spikes))
    return finish(False, (parts, levels, lines, ny), (solved, other, offsb, spikes), half_out)


def solution(mesh):
    return jax.shard_map(
        body,
        mesh=mesh,
        in_specs=(
            P(None, "depth", "horiz", None),
            P("depth", "horiz", None),
            P("horiz"),
            P(None, "depth"),
            P(None, "depth", None),
        ),
        out_specs=P(None, "depth", "horiz", None),
        check_vma=False,
    )
```
